512 devices in a mesh: dp: 128 (over z, y, core), expert: 4 (over x).
Axes of the slice: x: 4, y: 8, z: 8, core: 2. Of those that a mesh axis runs over, the one named last changes fastest.
Arguments:
- expert_grads: bfloat16 [128, 4, 1024, 896], P('dp', 'expert'), may hold values from -768 to 768
- round_offsets: int32 [128, 4, 1024], P('dp', 'expert'), may hold values from 0 to 1073741823
- slot_expert: int32 [4], replicated, may hold values from 0 to 3, each once
- master_weight: float32 [4, 1024, 896], P('expert', 'dp'), may hold values from -0.1875 to 0.1875
Outputs:
- mean_grad: float32 [4, 1024, 896], P('expert', 'dp')
- new_weight: float32 [4, 1024, 896], P('expert', 'dp')
- block_step: float32 [4, 128], P('expert', 'dp')
The draws below stay inside these ranges and needn't reach their ends.
Inputs may be any that keep to these rules, and one draw needn't show every extreme that they name: `slot_expert`: each of 0 to 3 appears once.
All inputs are finite; a program needn't handle non-finite values.
Results may differ from the reference program's by a relative error of at most 0.0003.
Values may be sent and summed in bfloat16 or wider, within the bound.
A program may use at most 64 MiB of HBM per device.

```python
import jax
import jax.numpy as jnp
from jax import lax

D = 1024
FF = 896
EXPERTS = 4
REPLICAS = 128
N_DP = 128


def draw_expert_grads(key, part):
    base_key = jax.random.fold_in(key, 11)
    scale_key = jax.random.fold_in(key, 12)
    pair_key = jax.random.fold_in(key, 13)
    block_count = REPLICAS
    block_rows = D // REPLICAS
    base = jnp.clip(jax.random.normal(base_key, (REPLICAS, EXPERTS, D, FF), jnp.float32), -4.0, 4.0)
    block_scale = jnp.exp(jax.random.uniform(scale_key, (EXPERTS, block_count), jnp.float32, jnp.log(0.5), jnp.log(32.0)))
    row_scale = jnp.repeat(block_scale, block_rows, axis=1)
    paired = jax.random.permutation(pair_key, block_count)
    blocks_iota = jnp.arange(block_count)
    spike = jnp.where(blocks_iota[None, :] == paired[:, None], jnp.float32(6.0), jnp.float32(1.0))
    row_spike = jnp.repeat(spike, block_rows, axis=1)
    values = base * row_scale[None, :, :, None] * row_spike[:, None, :, None]
    return values.astype(jnp.bfloat16)


def with_ends(drawn, own_key, smallest, high):
    longest = drawn.shape.index(max(drawn.shape))
    spots = []
    for shift in (0, 1):
        where = [jax.random.randint(jax.random.fold_in(own_key, axis), (), 0, length) for axis, length in enumerate(drawn.shape)]
        where[longest] = (where[longest] + shift) % drawn.shape[longest]
        spots.append(tuple(where))
    return drawn.at[spots[0]].set(smallest).at[spots[1]].set(high)


def steps_of(own_key, extent, pieces, smallest, top_value):
    gain = 1.0
    for dim, blocks in pieces:
        draws = jax.random.uniform(jax.random.fold_in(jax.random.fold_in(own_key, 6), dim), (blocks,), jnp.float32, smallest / len(pieces), top_value / len(pieces))
        gain = gain * jnp.repeat(jnp.exp(draws), extent[dim] // blocks).reshape((-1,) + (1,) * (len(extent) - 1 - dim))
    return gain


def gaussian(key, shape, deviation, limit, pieces=(), held_as=jnp.bfloat16):
    level = steps_of(key, shape, pieces, -0.22, 0.18) if pieces else 1.0
    values = jax.random.normal(key, shape, jnp.float32) * deviation * level
    return jnp.minimum(jnp.maximum(values, -limit), limit).astype(held_as)


def setup_inputs(seed: int = 0) -> dict:
    key_of = jax.random.split(jax.random.key(seed), 5)
    return {
        "expert_grads": draw_expert_grads(jax.random.fold_in(key_of[4], 71), 0),
        "round_offsets": with_ends(jax.random.randint(key_of[1], (REPLICAS, EXPERTS, D), 0, 2 ** 30), jax.random.fold_in(key_of[1], 1), 0, (2 ** 30) - 1).astype(jnp.int32),
        "slot_expert": jax.random.permutation(key_of[2], EXPERTS).astype(jnp.int32),
        "master_weight": gaussian(key_of[3], (EXPERTS, D, FF), D ** -0.5, 0.1875, ((0, 4), (1, 128)), jnp.float32),
    }


level_bits = 6
low_power = -30
high_power = 30
learn_rate = 0.05


def power_steps(maxima):
    powers = jnp.array([2.0 ** exponent for exponent in range(low_power, high_power)], jnp.float32)
    reached = maxima[..., None] >= powers
    doubled = jnp.prod(jnp.where(reached, jnp.float32(2.0), jnp.float32(1.0)), axis=-1)
    return (2.0 ** (low_power - level_bits)) * doubled


def dither(element_code):
    mixed = element_code * 747796405 + 1013904223
    mixed = jnp.bitwise_xor(mixed, jnp.right_shift(mixed, 13))
    mixed = mixed * 1103515245
    mixed = jnp.bitwise_xor(mixed, jnp.right_shift(mixed, 16))
    return jnp.bitwise_and(jnp.right_shift(mixed, 12), 255).astype(jnp.float32) / 256.0


def quantize(values, inverse_step, offsets):
    columns = lax.broadcasted_iota(jnp.int32, (1, values.shape[-1]), 1)
    element_code = offsets.astype(jnp.int32)[..., None] + columns
    scaled = values * inverse_step
    floor_part = jnp.floor(scaled)
    return (floor_part + jnp.floor((scaled - floor_part) + dither(element_code))).astype(jnp.int32)


def reference(expert_grads, round_offsets, slot_expert, master_weight):
    slot_count = expert_grads.shape[1]
    row_count = expert_grads.shape[2]
    hidden = expert_grads.shape[3]
    blocks = N_DP
    block_rows = row_count // blocks

    def max_step(running, grads_one):
        shaped = jnp.abs(grads_one).reshape(slot_count, blocks, block_rows, hidden)
        return jnp.maximum(running, jnp.max(shaped, axis=(2, 3)).astype(jnp.float32)), None

    maxima, ignored = lax.scan(max_step, jnp.zeros((slot_count, blocks), jnp.float32), expert_grads)
    step_sizes = power_steps(maxima)
    inverse_step = (1.0 / step_sizes)[:, :, None, None]

    def sum_step(running, grads_pair):
        grads_one, offsets_one = grads_pair
        shaped = grads_one.astype(jnp.float32).reshape(slot_count, blocks, block_rows, hidden)
        offsets_shaped = offsets_one.reshape(slot_count, blocks, block_rows)
        counts = quantize(shaped, inverse_step, offsets_shaped).reshape(slot_count, row_count, hidden)
        return running + counts, None

    totals, ignored = lax.scan(sum_step, jnp.zeros((slot_count, row_count, hidden), jnp.int32), (expert_grads, round_offsets))
    shaped_totals = totals.astype(jnp.float32).reshape(slot_count, blocks, block_rows, hidden)
    mean_slot = (shaped_totals * (step_sizes / N_DP)[:, :, None, None]).reshape(slot_count, row_count, hidden)
    inverse_order = jnp.argsort(slot_expert).astype(jnp.int32)
    mean_grad = mean_slot[inverse_order]
    block_step = step_sizes[inverse_order]
    new_weight = master_weight - learn_rate * mean_grad
    return mean_grad, new_weight, block_step
```

```python
import jax
import jax.numpy as jnp
from jax import lax
from jax.experimental import pallas as pl
from jax.experimental.pallas import tpu as pltpu
from jax.sharding import Mesh
from jax.sharding import PartitionSpec as P

DP = ("dp_0", "dp_1", "dp_2")
MESH = pl.DeviceIdType.MESH
A = 8
X = 4
ROWS = 8
COLS = 896
TILES = COLS // 128
CHUNKS = 4
low_power = -30
high_power = 30
learn_rate = 0.05
HASH_MUL = 747796405
HASH_ADD = 1013904223
HASH_MIX = 1103515245


def order(k):
    return 4 + ((k + 1) // 2) * (2 * ((k + 1) % 2) - 1)


def kernel(
    g_hbm, off_ref, se_ref, mw_ref, mean_o, new_o, step_o,
    gv, rp, poff, pm, mxs, rm1, mxs2, rm2, inv_s, stp_s, ob, pb, sums, rc1, acc, rc2, xs, rx,
    ld, sd, rd, sm1, sr1, sm2, sr2, s1, r1, s2, r2, sx, rxs,
):
    z, y, c, x = (lax.axis_index(n) for n in ("dp_0", "dp_1", "dp_2", "expert"))
    a = y + c * (z - y)
    b = z + c * (y - z)

    def peer_a(ap):
        return (z + c * (ap - z), ap + c * (y - ap), c, x)

    def peer_b(bp):
        return (bp + c * (z - bp), y + c * (bp - y), c, x)

    def rdma(src, dst, send, recv, dev):
        return pltpu.make_async_remote_copy(
            src_ref=src, dst_ref=dst, send_sem=send, recv_sem=recv, device_id=dev, device_id_type=MESH
        )

    partner = (z, y, 1 - c, x)
    per = A * A // CHUNKS

    def load(q, h):
        rows = pl.ds(q * per, per)
        return pltpu.make_async_copy(g_hbm.at[rows, h], gv.at[h, rows], ld.at[q, h])

    for q in range(CHUNKS):
        for h in range(2):
            load(q, h).start()

    barrier = pltpu.get_barrier_semaphore()
    me16 = y * 2 + c

    def greet16(k, carry):
        p = (me16 + k) % (2 * A)
        pl.semaphore_signal(barrier, inc=1, device_id=(z, p // 2, p % 2, x), device_id_type=MESH)
        return carry

    def greet8(k, carry):
        pl.semaphore_signal(barrier, inc=1, device_id=((z + k) % A, y, c, x), device_id_type=MESH)
        return carry

    def greet4(k, carry):
        pl.semaphore_signal(barrier, inc=1, device_id=(z, y, c, (x + k) % X), device_id_type=MESH)
        return carry

    lax.fori_loop(1, 2 * A, greet16, 0)
    lax.fori_loop(1, A, greet8, 0)
    lax.fori_loop(1, X, greet4, 0)

    for q in range(CHUNKS):
        for h in range(2):
            load(q, h).wait()

            def block_max(i, carry):
                v = jnp.abs(gv[h, i].astype(jnp.float32))
                m = v[:, :128]
                for t in range(1, TILES):
                    m = jnp.maximum(m, v[:, t * 128 : (t + 1) * 128])
                pm[pl.ds((h * A * A + i) * ROWS, ROWS), :] = m
                return carry

            lax.fori_loop(q * per, (q + 1) * per, block_max, 0, unroll=2)
    top = pm[pl.ds(0, 128, stride=ROWS), :]
    for r in range(1, ROWS):
        top = jnp.maximum(top, pm[pl.ds(r, 128, stride=ROWS), :])
    mine = jnp.max(top.T, axis=0, keepdims=True)
    mxs[...] = mine
    rm1[me16] = mine

    pl.semaphore_wait(barrier, (2 * A - 1) + (A - 1) + (X - 1))

    def send_max(k, carry):
        p = (me16 + k) % (2 * A)
        rdma(mxs, rm1.at[me16], sm1.at[p], sr1.at[me16], (z, p // 2, p % 2, x)).start()
        return carry

    lax.fori_loop(1, 2 * A, send_max, 0)
    raw = rdma(gv.at[1 - c], rp, sd.at[0], rd.at[0], partner)
    raw_off = rdma(off_ref, poff, sd.at[1], rd.at[1], partner)
    raw_off.start()
    raw.start()

    def spread(ref, out):
        start = ref[...] * HASH_MUL + HASH_ADD
        for i in range(A):
            wide = jnp.broadcast_to(start[i : i + 1, :], (128, 128)).T
            out[pl.ds(i * 128, 128), :] = wide

    spread(off_ref, ob)

    def wait_max(k, carry):
        p = (me16 + k) % (2 * A)
        rdma(mxs, rm1.at[p], sm1.at[p], sr1.at[p], partner).wait_recv()
        return carry

    lax.fori_loop(1, 2 * A, wait_max, 0)
    ring = jnp.max(rm1[...], axis=0)
    mxs2[...] = ring
    rm2[z] = ring

    def send_max2(k, carry):
        p = (z + k) % A
        rdma(mxs2, rm2.at[z], sm2.at[p], sr2.at[z], (p, y, c, x)).start()
        return carry

    lax.fori_loop(1, A, send_max2, 0)
    raw_off.wait_recv()
    spread(poff, pb)

    def wait_max2(k, carry):
        p = (z + k) % A
        rdma(mxs2, rm2.at[p], sm2.at[p], sr2.at[p], partner).wait_recv()
        return carry

    lax.fori_loop(1, A, wait_max2, 0)
    best = jnp.max(rm2[...], axis=0)
    step = jnp.full((1, 128), 2.0 ** (low_power - 6), jnp.float32)
    inverse = jnp.full((1, 128), 2.0 ** (6 - low_power + 20), jnp.float32)
    for e in range(low_power, high_power):
        over = best >= 2.0**e
        step = jnp.where(over, jnp.float32(2.0 ** (e - 5)), step)
        inverse = jnp.where(over, jnp.float32(2.0 ** (25 - e)), inverse)
    inv_s[...] = jnp.broadcast_to(inverse, (128, 128)).T
    stp_s[...] = jnp.broadcast_to(step, (128, 128)).T

    lane = lax.broadcasted_iota(jnp.int32, (ROWS, 128), 1)
    column = [(lane + t * 128) * HASH_MUL for t in range(TILES)]
    raw.wait_recv()

    def rounded(tile, inverse, noise):
        whole = jnp.floor(tile.astype(jnp.float32) * inverse).astype(jnp.int32)
        noise = noise ^ (noise >> 13)
        noise = noise * HASH_MIX
        noise = noise ^ (noise >> 16)
        return (whole + (noise & 0xFF000)) >> 20

    def first_send(ap):
        return rdma(sums.at[ap], rc1.at[a], s1.at[ap], r1.at[a], peer_a(ap))

    def quantize_chunk(ap):
        def one(bp, carry):
            zy = ap * (1 + 7 * c) + bp * (8 - 7 * c)
            inverse = jnp.broadcast_to(inv_s[pl.ds(c * A * A + zy, 1), :], (ROWS, 128))
            rows = pl.ds((zy * 2 + c) * ROWS, ROWS)
            mine, theirs = ob[rows, :], pb[rows, :]
            for t in range(TILES):
                cols = pl.ds(t * 128, 128)
                both = rounded(gv[c, zy, :, cols], inverse, mine + column[t])
                both += rounded(rp[zy, :, cols], inverse, theirs + column[t])
                sums[ap, bp, :, cols] = both.astype(jnp.float32).astype(jnp.bfloat16)
            return carry

        lax.fori_loop(0, A, one, 0)

    def quantize_send(k, carry):
        ap = (a + order(k)) % A
        quantize_chunk(ap)
        first_send(ap).start()
        return carry

    lax.fori_loop(0, A - 1, quantize_send, 0)
    quantize_chunk(a)

    def clear(bp, carry):
        acc[bp] = sums[a, bp].astype(jnp.float32)
        return carry

    lax.fori_loop(0, A, clear, 0)

    def gather_first(k, carry):
        ap = (a - order(k) + A) % A
        rdma(sums.at[0], rc1.at[ap], s1.at[ap], r1.at[ap], partner).wait_recv()

        def add(bp, inner):
            acc[bp] += rc1[ap, bp].astype(jnp.float32)
            return inner

        lax.fori_loop(0, A, add, 0)
        return carry

    lax.fori_loop(0, A - 1, gather_first, 0)

    def second_send(k, carry):
        bp = (b + order(k)) % A
        rdma(acc.at[bp], rc2.at[b], s2.at[bp], r2.at[b], peer_b(bp)).start()
        return carry

    lax.fori_loop(0, A - 1, second_send, 0)
    rc2[b] = acc[b]

    def gather_second(k, carry):
        bp = (b - order(k) + A) % A
        rdma(acc.at[0], rc2.at[bp], s2.at[bp], r2.at[bp], partner).wait_recv()
        return carry

    lax.fori_loop(0, A - 1, gather_second, 0)
    own = stp_s[pl.ds(c * A * A + z * A + y, 1), :]
    total = rc2[0]
    for i in range(1, A):
        total += rc2[i]
    own8 = jnp.broadcast_to(own, (ROWS, 128))
    share = own8 * (1.0 / (2 * A * A))
    for t in range(TILES):
        xs[:, t * 128 : (t + 1) * 128] = total[:, t * 128 : (t + 1) * 128] * share
    xs[:, COLS:] = own8

    def send_x(k, carry):
        xp = (x + k) % X
        rdma(xs, rx.at[x], sx.at[xp], rxs.at[x], (z, y, c, xp)).start()
        return carry

    lax.fori_loop(1, X, send_x, 0)
    rx[x] = xs[...]

    def wait_x(k, carry):
        xp = (x + k) % X
        rdma(xs, rx.at[xp], sx.at[xp], rxs.at[xp], partner).wait_recv()
        return carry

    lax.fori_loop(1, X, wait_x, 0)
    value = rx[X - 1]
    for s in range(X - 1):
        value = jnp.where(se_ref[s] == x, rx[s], value)
    mean = value[:, :COLS]
    mean_o[...] = mean
    new_o[...] = mw_ref[...] - learn_rate * mean
    step_o[...] = value[0:1, COLS : COLS + 1]

    raw.wait_send()
    raw_off.wait_send()

    def drain16(k, carry):
        p = (me16 + k) % (2 * A)
        rdma(mxs, rm1.at[me16], sm1.at[p], sr1.at[me16], partner).wait_send()
        return carry

    lax.fori_loop(1, 2 * A, drain16, 0)

    def drain8(k, carry):
        rdma(mxs2, rm2.at[z], sm2.at[(z + k) % A], sr2.at[z], partner).wait_send()
        rdma(sums.at[0], rc1.at[a], s1.at[(a + k) % A], r1.at[a], partner).wait_send()
        rdma(acc.at[0], rc2.at[b], s2.at[(b + k) % A], r2.at[b], partner).wait_send()
        return carry

    lax.fori_loop(1, A, drain8, 0)

    def drain4(k, carry):
        rdma(xs, rx.at[x], sx.at[(x + k) % X], rxs.at[x], partner).wait_send()
        return carry

    lax.fori_loop(1, X, drain4, 0)


def body(expert_grads, round_offsets, slot_expert, master_weight):
    n = A * A
    f32, bf16, i32 = jnp.float32, jnp.bfloat16, jnp.int32
    dma = pltpu.SemaphoreType.DMA
    vmem = pl.BlockSpec(memory_space=pltpu.VMEM)
    mean, new, step = pl.pallas_call(
        kernel,
        name="average",
        out_shape=(
            jax.ShapeDtypeStruct((ROWS, COLS), f32),
            jax.ShapeDtypeStruct((ROWS, COLS), f32),
            jax.ShapeDtypeStruct((1, 1), f32),
        ),
        in_specs=[
            pl.BlockSpec(memory_space=pl.ANY),
            vmem,
            pl.BlockSpec(memory_space=pltpu.SMEM),
            vmem,
        ],
        out_specs=(vmem, vmem, vmem),
        scratch_shapes=[
            pltpu.VMEM((2, n, ROWS, COLS), bf16),
            pltpu.VMEM((n, ROWS, COLS), bf16),
            pltpu.VMEM((A, 128), i32),
            pltpu.VMEM((2 * n * ROWS, 128), f32),
            pltpu.VMEM((1, 128), f32),
            pltpu.VMEM((2 * A, 1, 128), f32),
            pltpu.VMEM((1, 128), f32),
            pltpu.VMEM((A, 1, 128), f32),
            pltpu.VMEM((128, 128), f32),
            pltpu.VMEM((128, 128), f32),
            pltpu.VMEM((2 * n * ROWS, 128), i32),
            pltpu.VMEM((2 * n * ROWS, 128), i32),
            pltpu.VMEM((A, A, ROWS, COLS), bf16),
            pltpu.VMEM((A, A, ROWS, COLS), bf16),
            pltpu.VMEM((A, ROWS, COLS), f32),
            pltpu.VMEM((A, ROWS, COLS), f32),
            pltpu.VMEM((ROWS, COLS + 128), f32),
            pltpu.VMEM((X, ROWS, COLS + 128), f32),
            dma((CHUNKS, 2)),
            dma((2,)),
            dma((2,)),
            dma((2 * A,)),
            dma((2 * A,)),
            dma((A,)),
            dma((A,)),
            dma((A,)),
            dma((A,)),
            dma((A,)),
            dma((A,)),
            dma((X,)),
            dma((X,)),
        ],
        compiler_params=pltpu.CompilerParams(collective_id=0, has_side_effects=True),
    )(
        expert_grads.reshape(n, 2, ROWS, COLS),
        round_offsets.reshape(A, 128),
        slot_expert,
        master_weight.reshape(ROWS, COLS),
    )
    return mean[None], new[None], step


def solution(mesh):
    finer = Mesh(
        mesh.devices.reshape(A, A, 2, mesh.shape["expert"]), ("dp_0", "dp_1", "dp_2", "expert")
    )
    return jax.shard_map(
        body,
        mesh=finer,
        in_specs=(P(DP, "expert", None, None), P(DP, "expert", None), P(), P("expert", DP, None)),
        out_specs=(P("expert", DP, None), P("expert", DP, None), P("expert", DP)),
        check_vma=False,
    )
```

```python
import jax
import jax.numpy as jnp
from jax import lax
from jax.experimental import pallas as pl
from jax.experimental.pallas import tpu as pltpu
from jax.sharding import Mesh
from jax.sharding import PartitionSpec as P

DP = ("dp_0", "dp_1", "dp_2")
MESH = pl.DeviceIdType.MESH
A = 8
X = 4
H = A // 2
ROWS = 8
COLS = 896
TILES = COLS // 128
CHUNKS = 4
low_power = -30
high_power = 30
learn_rate = 0.05
HASH_MUL = 747796405
HASH_ADD = 1013904223
HASH_MIX = 1103515245


def order(k):
    return 4 + ((k + 1) // 2) * (2 * ((k + 1) % 2) - 1)


def kernel(
    g_hbm, off_hbm, rx,
    gv, rp, offv, roff, toff, obs, pm, mxs, rm1, mxs2, rm2, inv_s, stp_s, sums, rc1, acc, rc2,
    ld, lo, so, ro, sraw, rr, sm1, sr1, sm2, sr2, s1, r1, s2, r2, sx, rxs,
):
    z, y, c, x = (lax.axis_index(n) for n in ("dp_0", "dp_1", "dp_2", "expert"))
    a = y + c * (z - y)
    b = z + c * (y - z)

    def peer_a(ap):
        return (z + c * (ap - z), ap + c * (y - ap), c, x)

    def peer_b(bp):
        return (bp + c * (z - bp), y + c * (bp - y), c, x)

    def rdma(src, dst, send, recv, dev):
        return pltpu.make_async_remote_copy(
            src_ref=src, dst_ref=dst, send_sem=send, recv_sem=recv, device_id=dev, device_id_type=MESH
        )

    partner = (z, y, 1 - c, x)
    per = A // CHUNKS

    def way(position, h):
        return 2 * ((position + h) & 1) - 1

    def load(q, h):
        rows = pl.ds(q * per, per)
        return pltpu.make_async_copy(g_hbm.at[rows, :, h], gv.at[h, rows], ld.at[q, h])

    load_off = pltpu.make_async_copy(off_hbm, offv, lo.at[0])
    load_off.start()
    for q in range(CHUNKS):
        for h in range(2):
            load(q, h).start()

    barrier = pltpu.get_barrier_semaphore()
    me16 = y * 2 + c

    def greet(dev):
        pl.semaphore_signal(barrier, inc=1, device_id=dev, device_id_type=MESH)

    def greet16(k, carry):
        p = (me16 + k) & 15
        greet((z, p >> 1, p & 1, x))
        return carry

    def greet8(k, carry):
        greet(((z + k) & 7, y, c, x))
        return carry

    def greet4(k, carry):
        greet((z, y, c, (x + k) & 3))
        return carry

    lax.fori_loop(1, 2 * A, greet16, 0)
    lax.fori_loop(1, A, greet8, 0)
    lax.fori_loop(1, X, greet4, 0)
    greet(((z + 1) & 7, y, 1 - c, x))
    greet(((z + 7) & 7, y, 1 - c, x))

    for q in range(CHUNKS):
        for h in range(2):
            load(q, h).wait()

            def block_max(i, carry):
                v = jnp.abs(gv[h, i >> 3, i & 7].astype(jnp.float32))
                m = v[:, :128]
                for t in range(1, TILES):
                    m = jnp.maximum(m, v[:, t * 128 : (t + 1) * 128])
                pm[pl.ds((h * A * A + i) * ROWS, ROWS), :] = m
                return carry

            lax.fori_loop(q * per * A, (q + 1) * per * A, block_max, 0, unroll=4)
    top = pm[pl.ds(0, 128, stride=ROWS), :]
    for r in range(1, ROWS):
        top = jnp.maximum(top, pm[pl.ds(r, 128, stride=ROWS), :])
    mine = jnp.max(top.T, axis=0, keepdims=True)
    mxs[...] = mine
    rm1[me16] = mine
    load_off.wait()

    pl.semaphore_wait(barrier, (2 * A - 1) + (A - 1) + (X - 1) + 2)

    def send_max(k, carry):
        p = (me16 + k) & 15
        rdma(mxs, rm1.at[me16], sm1.at[p], sr1.at[me16], (z, p >> 1, p & 1, x)).start()
        return carry

    lax.fori_loop(1, 2 * A, send_max, 0)

    halves = [pl.ds(h * H, H) for h in range(2)]

    def raw_rows(core, position, h):
        return gv.at[core, halves[h], position] if core == 0 else gv.at[core, position, halves[h]]

    rdma(offv, roff.at[0], so.at[0], ro.at[0], partner).start()
    for core, position in ((0, y), (1, z)):
        for h in range(2):
            near = (position - way(position, h)) & 7
            dev = (z, near, 0, x) if core == 0 else (near, y, 1, x)
            slot = 1 + 2 * h + c
            rdma(offv, roff.at[slot], so.at[1 + 2 * core + h], ro.at[slot], dev).start()
            for m in range(H):
                dest = (position - way(position, h) * (1 + m)) & 7
                rdma(
                    raw_rows(core, dest, h), rp.at[1 + c, m, halves[h]], sraw.at[core, h, m], rr.at[1 + c, h, m], dev
                ).start()

        @pl.when(c != core)
        def _():
            for h in range(2):
                for m in range(H):
                    dest = (position + way(position, h) * m) & 7
                    rdma(
                        raw_rows(core, dest, h), rp.at[0, m, halves[h]], sraw.at[2, h, m], rr.at[0, h, m], partner
                    ).start()

    def turned(value, slot):
        start = value * HASH_MUL + HASH_ADD
        toff[slot] = jnp.concatenate([start] * 16, axis=0).T

    def block_of(m, bp, h):
        ap = (a + way(a, h) * m) & 7
        return bp + c * (ap - bp), ap + c * (bp - ap)

    def spread(which, slots):
        for m in range(H):
            for bp in range(A):
                zp, yp = block_of(m, bp, bp // H)
                tile = toff[slots[bp // H], pl.ds((yp * 2 + c) * ROWS, ROWS), :]
                index = jnp.full((ROWS, 128), zp, jnp.int32)
                obs[which, m, bp] = jnp.take_along_axis(tile, index, axis=1, mode="promise_in_bounds")

    turned(offv[...], 5)
    spread(0, (5, 5))

    def wait_max(k, carry):
        p = (me16 + k) & 15
        rdma(mxs, rm1.at[p], sm1.at[p], sr1.at[p], partner).wait_recv()
        return carry

    lax.fori_loop(1, 2 * A, wait_max, 0)
    ring = jnp.max(rm1[...], axis=0)
    mxs2[...] = ring
    rm2[z] = ring

    def send_max2(k, carry):
        p = (z + k) & 7
        rdma(mxs2, rm2.at[z], sm2.at[p], sr2.at[z], (p, y, c, x)).start()
        return carry

    lax.fori_loop(1, A, send_max2, 0)
    for i in range(5):
        rdma(offv, roff.at[i], so.at[0], ro.at[i], partner).wait_recv()
        turned(roff[i], i)
    spread(1, (0, 0))
    spread(2, (1, 3))
    spread(3, (2, 4))

    def wait_max2(k, carry):
        p = (z + k) & 7
        rdma(mxs2, rm2.at[p], sm2.at[p], sr2.at[p], partner).wait_recv()
        return carry

    lax.fori_loop(1, A, wait_max2, 0)
    best = jnp.broadcast_to(jnp.max(rm2[...], axis=0), (ROWS, 128))
    step = jnp.full((ROWS, 128), 2.0 ** (low_power - 6), jnp.float32)
    inverse = jnp.full((ROWS, 128), 2.0 ** (6 - low_power + 20), jnp.float32)
    for e in range(low_power, high_power):
        over = best >= 2.0**e
        step = jnp.where(over, jnp.float32(2.0 ** (e - 5)), step)
        inverse = jnp.where(over, jnp.float32(2.0 ** (25 - e)), inverse)
    inv_s[...] = inverse
    stp_s[...] = step

    lane = lax.broadcasted_iota(jnp.int32, (ROWS, 128), 1)
    column = [(lane + t * 128) * HASH_MUL for t in range(TILES)]

    def rounded(tile, scale, noise):
        whole = jnp.floor(tile.astype(jnp.float32) * scale).astype(jnp.int32)
        noise = noise ^ (noise >> 13)
        noise = noise * HASH_MIX
        noise = noise ^ (noise >> 16)
        return (whole + (noise & 0xFF000)) >> 20

    def pick(ref, block):
        index = jnp.full((ROWS, 128), block, jnp.int32)
        return jnp.take_along_axis(ref[...], index, axis=1, mode="promise_in_bounds")

    def first_send(h, m):
        half = halves[h]
        return rdma(
            sums.at[m, half], rc1.at[m - 1, half], s1.at[h, m - 1], r1.at[h, m - 1], peer_a((a + way(a, h) * m) & 7)
        )

    for m in range(H - 1, -1, -1):
        for h in range(2):
            for j in range(3):
                rdma(rp.at[j, m, halves[h]], rp.at[j, m, halves[h]], sraw.at[0, h, m], rr.at[j, h, m], partner).wait_recv()

            def one(bp, carry):
                zp, yp = block_of(m, bp, h)
                scale = pick(inv_s, c * A * A + zp * A + yp)
                starts = [obs[j, m, bp] for j in range(4)]
                for t in range(TILES):
                    cols = pl.ds(t * 128, 128)
                    both = rounded(gv[c, zp, yp, :, cols], scale, starts[0] + column[t])
                    for j in range(3):
                        both += rounded(rp[j, m, bp, :, cols], scale, starts[1 + j] + column[t])
                    sums[m, bp, :, cols] = both.astype(jnp.float32).astype(jnp.bfloat16)
                return carry

            lax.fori_loop(h * H, (h + 1) * H, one, 0)
            if m:
                first_send(h, m).start()

    for h in range(2):
        for m in range(1, H):
            first_send(h, m).wait_recv()

        def add(bp, carry):
            total = sums[0, bp].astype(jnp.float32)
            for m in range(H - 1):
                total += rc1[m, bp].astype(jnp.float32)
            acc[bp] = total

            @pl.when(bp != b)
            def _():
                rdma(acc.at[bp], rc2.at[b], s2.at[bp], r2.at[b], peer_b(bp)).start()

            return carry

        lax.fori_loop(h * H, (h + 1) * H, add, 0)
    rc2[b] = acc[b]
    own = pick(stp_s, c * A * A + z * A + y)

    def gather_second(k, carry):
        bp = (b + k) & 7
        rdma(acc.at[bp], rc2.at[bp], s2.at[bp], r2.at[bp], partner).wait_recv()
        return carry

    lax.fori_loop(1, A, gather_second, 0)
    total = rc2[0]
    for i in range(1, A):
        total += rc2[i]
    share = own * (1.0 / (2 * A * A))
    for t in range(TILES):
        rx[x, :, t * 128 : (t + 1) * 128] = total[:, t * 128 : (t + 1) * 128] * share
    rx[x, :, COLS:] = own

    def send_x(k, carry):
        xp = (x + k) & 3
        rdma(rx.at[x], rx.at[x], sx.at[xp], rxs.at[x], (z, y, c, xp)).start()
        return carry

    lax.fori_loop(1, X, send_x, 0)

    for i in range(5):
        rdma(offv, roff.at[i], so.at[i], ro.at[i], partner).wait_send()
    for j in range(3):
        for h in range(2):
            for m in range(H):
                rdma(rp.at[j, m, halves[h]], rp.at[j, m, halves[h]], sraw.at[j, h, m], rr.at[j, h, m], partner).wait_send()
    for h in range(2):
        for m in range(1, H):
            first_send(h, m).wait_send()

    def drain16(k, carry):
        p = (me16 + k) & 15
        rdma(mxs, rm1.at[me16], sm1.at[p], sr1.at[me16], partner).wait_send()
        return carry

    lax.fori_loop(1, 2 * A, drain16, 0)

    def drain8(k, carry):
        rdma(mxs2, rm2.at[z], sm2.at[(z + k) & 7], sr2.at[z], partner).wait_send()
        bp = (b + k) & 7
        rdma(acc.at[bp], rc2.at[b], s2.at[bp], r2.at[b], partner).wait_send()
        return carry

    lax.fori_loop(1, A, drain8, 0)

    def wait_x(k, carry):
        xp = (x + k) & 3
        rdma(rx.at[xp], rx.at[xp], sx.at[xp], rxs.at[xp], partner).wait_recv()
        return carry

    lax.fori_loop(1, X, wait_x, 0)

    def drain4(k, carry):
        xp = (x + k) & 3
        rdma(rx.at[x], rx.at[x], sx.at[xp], rxs.at[x], partner).wait_send()
        return carry

    lax.fori_loop(1, X, drain4, 0)


def finish(rx, se_ref, mw_ref, mean_o, new_o, step_o):
    x = lax.axis_index("expert")
    value = rx[X - 1]
    for s in range(X - 1):
        value = jnp.where(se_ref[s] == x, rx[s], value)
    mean = value[:, :COLS]
    mean_o[...] = mean
    new_o[...] = mw_ref[...] - learn_rate * mean
    step_o[...] = value[0:1, COLS : COLS + 1]


def body(expert_grads, round_offsets, slot_expert, master_weight):
    f32, bf16, i32 = jnp.float32, jnp.bfloat16, jnp.int32
    dma = pltpu.SemaphoreType.DMA
    vmem = pl.BlockSpec(memory_space=pltpu.VMEM)
    hbm = pl.BlockSpec(memory_space=pl.ANY)
    gathered = pl.pallas_call(
        kernel,
        name="average",
        out_shape=pltpu.VMEM((X, ROWS, COLS + 128), f32),
        in_specs=[hbm, hbm],
        out_specs=vmem,
        scratch_shapes=[
            pltpu.VMEM((2, A, A, ROWS, COLS), bf16),
            pltpu.VMEM((3, H, A, ROWS, COLS), bf16),
            pltpu.VMEM((A, 128), i32),
            pltpu.VMEM((5, A, 128), i32),
            pltpu.VMEM((6, 128, 128), i32),
            pltpu.VMEM((4, H, A, ROWS, 128), i32),
            pltpu.VMEM((2 * A * A * ROWS, 128), f32),
            pltpu.VMEM((1, 128), f32),
            pltpu.VMEM((2 * A, 1, 128), f32),
            pltpu.VMEM((1, 128), f32),
            pltpu.VMEM((A, 1, 128), f32),
            pltpu.VMEM((ROWS, 128), f32),
            pltpu.VMEM((ROWS, 128), f32),
            pltpu.VMEM((H, A, ROWS, COLS), bf16),
            pltpu.VMEM((H - 1, A, ROWS, COLS), bf16),
            pltpu.VMEM((A, ROWS, COLS), f32),
            pltpu.VMEM((A, ROWS, COLS), f32),
            dma((CHUNKS, 2)),
            dma((1,)),
            dma((5,)),
            dma((5,)),
            dma((3, 2, H)),
            dma((3, 2, H)),
            dma((2 * A,)),
            dma((2 * A,)),
            dma((A,)),
            dma((A,)),
            dma((2, H - 1)),
            dma((2, H - 1)),
            dma((A,)),
            dma((A,)),
            dma((X,)),
            dma((X,)),
        ],
        compiler_params=pltpu.CompilerParams(collective_id=0, has_side_effects=True),
    )(expert_grads.reshape(A, A, 2, ROWS, COLS), round_offsets.reshape(A, 128))
    mean, new, step = pl.pallas_call(
        finish,
        name="finish",
        out_shape=(
            jax.ShapeDtypeStruct((ROWS, COLS), f32),
            jax.ShapeDtypeStruct((ROWS, COLS), f32),
            jax.ShapeDtypeStruct((1, 1), f32),
        ),
        in_specs=[vmem, pl.BlockSpec(memory_space=pltpu.SMEM), vmem],
        out_specs=(vmem, vmem, vmem),
        compiler_params=pltpu.CompilerParams(vmem_limit_bytes=1024 * 1024),
    )(gathered, slot_expert, master_weight.reshape(ROWS, COLS))
    return mean[None], new[None], step


def solution(mesh):
    finer = Mesh(
        mesh.devices.reshape(A, A, 2, mesh.shape["expert"]), ("dp_0", "dp_1", "dp_2", "expert")
    )
    return jax.shard_map(
        body,
        mesh=finer,
        in_specs=(P(DP, "expert", None, None), P(DP, "expert", None), P(), P("expert", DP, None)),
        out_specs=(P("expert", DP, None), P("expert", DP, None), P("expert", DP)),
        check_vma=False,
    )
```

```python
import jax
import jax.numpy as jnp
from jax import lax
from jax.experimental import pallas as pl
from jax.experimental.pallas import tpu as pltpu
from jax.sharding import Mesh
from jax.sharding import PartitionSpec as P

DP = ("dp_0", "dp_1", "dp_2")
MESH = pl.DeviceIdType.MESH
A = 8
X = 4
H = A // 2
ROWS = 8
COLS = 896
TILES = COLS // 128
CHUNKS = 4
low_power = -30
high_power = 30
learn_rate = 0.05
HASH_MUL = 747796405
HASH_ADD = 1013904223
HASH_MIX = 1103515245


def kernel(
    g_hbm, off_hbm, rx,
    gv, rp, offv, roff, toff, noise, pm, mxs, rm1, mxs2, rm2, stp_s, scl, sums, rc,
    ld, lo, so, ro, sraw, rr, sm1, sr1, sm2, sr2, s1, r1, sx, rxs,
):
    z, y, c, x = (lax.axis_index(n) for n in ("dp_0", "dp_1", "dp_2", "expert"))

    def rdma(src, dst, send, recv, dev):
        return pltpu.make_async_remote_copy(
            src_ref=src, dst_ref=dst, send_sem=send, recv_sem=recv, device_id=dev, device_id_type=MESH
        )

    partner = (z, y, 1 - c, x)
    per = A // CHUNKS

    def way(position, core):
        return 2 * ((position + core) & 1) - 1

    def load(q, h):
        rows = pl.ds(q * per, per)
        return pltpu.make_async_copy(g_hbm.at[rows, :, h], gv.at[h, rows], ld.at[q, h])

    load_off = pltpu.make_async_copy(off_hbm, offv, lo.at[0])
    load_off.start()
    for q in range(CHUNKS):
        for h in range(2):
            load(q, h).start()

    barrier = pltpu.get_barrier_semaphore()
    me16 = y * 2 + c
    mz16 = z * 2 + c

    def greet(dev):
        pl.semaphore_signal(barrier, inc=1, device_id=dev, device_id_type=MESH)

    def greet16(k, carry):
        p = (me16 + k) & 15
        greet((z, p >> 1, p & 1, x))
        return carry

    def greet14(k, carry):
        p = (mz16 + k) & 15

        @pl.when((p >> 1) != z)
        def _():
            greet((p >> 1, y, p & 1, x))

        return carry

    def greet4(k, carry):
        greet((z, y, c, (x + k) & 3))
        return carry

    def near(position, core):
        return (position - way(position, core)) & 7

    lax.fori_loop(1, 2 * A, greet16, 0)
    lax.fori_loop(1, 2 * A, greet14, 0)
    lax.fori_loop(1, X, greet4, 0)
    greet((near(z, c), near(y, c), c, x))
    greet((near(z, c), near(y, c), 1 - c, x))
    greet((near(z, 1 - c), near(y, 1 - c), 1 - c, x))

    for q in range(CHUNKS):
        for h in range(2):
            load(q, h).wait()

            def block_max(i, carry):
                v = jnp.abs(gv[h, i >> 3, i & 7].astype(jnp.float32))
                m = v[:, :128]
                for t in range(1, TILES):
                    m = jnp.maximum(m, v[:, t * 128 : (t + 1) * 128])
                pm[pl.ds((h * A * A + i) * ROWS, ROWS), :] = m
                return carry

            lax.fori_loop(q * per * A, (q + 1) * per * A, block_max, 0, unroll=4)
    top = pm[pl.ds(0, 128, stride=ROWS), :]
    for r in range(1, ROWS):
        top = jnp.maximum(top, pm[pl.ds(r, 128, stride=ROWS), :])
    mine = jnp.max(top.T, axis=0, keepdims=True)
    mxs[...] = mine
    rm1[me16] = mine
    load_off.wait()

    pl.semaphore_wait(barrier, (2 * A - 1) + (2 * A - 2) + (X - 1) + 3)

    def send_max(k, carry):
        p = (me16 + k) & 15
        rdma(mxs, rm1.at[me16], sm1.at[p], sr1.at[me16], (z, p >> 1, p & 1, x)).start()
        return carry

    lax.fori_loop(1, 2 * A, send_max, 0)

    def to_near(core, q):
        return (near(z, core) if q else z, y if q == 1 else near(y, core), core, x)

    def dest(position, core, away, m):
        return (position + way(position, core) * ((-1 - m) if away else m)) & 7

    rdma(offv, roff.at[0], so.at[0], ro.at[0], partner).start()
    for core in range(2):
        for q in range(3):
            slot = 1 + 2 * q + c
            rdma(offv, roff.at[slot], so.at[1 + 3 * core + q], ro.at[slot], to_near(core, q)).start()

    def raw_part(first):
        def one(i, carry):
            mz, my = (i >> 2), i & 3
            for core in range(2):
                for q in (2, 1, 0):
                    src = gv.at[core, dest(z, core, q > 0, mz), dest(y, core, q != 1, my)]
                    slot = 1 + 2 * q + c
                    rdma(src, rp.at[slot, mz, my], sraw.at[3 * core + q], rr.at[slot, mz], to_near(core, q)).start()
            src = gv.at[1 - c, dest(z, 1 - c, False, mz), dest(y, 1 - c, False, my)]
            rdma(src, rp.at[0, mz, my], sraw.at[6], rr.at[0, mz], partner).start()
            return carry

        lax.fori_loop(first, first + 2 * H, one, 0)

    raw_part(2 * H)

    lane = lax.broadcasted_iota(jnp.int32, (ROWS, 128), 1)
    column = [(lane + t * 128) * HASH_MUL for t in range(TILES)]

    def dither(j, value):
        start = value * HASH_MUL + HASH_ADD
        toff[j] = jnp.concatenate([start] * 16, axis=0).T

        def one(mz, carry):
            zp = dest(z, c, False, mz)
            index = jnp.full((ROWS, 128), zp, jnp.int32)
            for my in range(H):
                yp = dest(y, c, False, my)
                tile = toff[j, pl.ds((yp * 2 + c) * ROWS, ROWS), :]
                code = jnp.take_along_axis(tile, index, axis=1, mode="promise_in_bounds")
                for t in range(TILES):
                    v = code + column[t]
                    v = v ^ (v >> 13)
                    v = v * HASH_MIX
                    v = v ^ (v >> 16)
                    noise[j, mz, my, :, pl.ds(t * 128, 128)] = v & 0xFF000
            return carry

        lax.fori_loop(0, H, one, 0)

    dither(7, offv[...])

    def wait_max(k, carry):
        p = (me16 + k) & 15
        rdma(mxs, rm1.at[p], sm1.at[p], sr1.at[p], partner).wait_recv()
        return carry

    lax.fori_loop(1, 2 * A, wait_max, 0)
    ring = jnp.max(rm1[...], axis=0)
    mxs2[...] = ring
    rm2[z] = ring

    def send_max2(k, carry):
        p = (z + k) & 7
        rdma(mxs2, rm2.at[z], sm2.at[p], sr2.at[z], (p, y, c, x)).start()
        return carry

    lax.fori_loop(1, A, send_max2, 0)
    raw_part(0)
    for j in range(7):
        rdma(offv, roff.at[j], so.at[0], ro.at[j], partner).wait_recv()
        dither(j, roff[j])

    def wait_max2(k, carry):
        p = (z + k) & 7
        rdma(mxs2, rm2.at[p], sm2.at[p], sr2.at[p], partner).wait_recv()
        return carry

    lax.fori_loop(1, A, wait_max2, 0)
    best = jnp.broadcast_to(jnp.max(rm2[...], axis=0), (ROWS, 128))
    step = jnp.full((ROWS, 128), 2.0 ** (low_power - 6), jnp.float32)
    inverse = jnp.full((ROWS, 128), 2.0 ** (6 - low_power + 20), jnp.float32)
    for e in range(low_power, high_power):
        over = best >= 2.0**e
        step = jnp.where(over, jnp.float32(2.0 ** (e - 5)), step)
        inverse = jnp.where(over, jnp.float32(2.0 ** (25 - e)), inverse)

    def pick(value, block):
        index = jnp.full((ROWS, 128), block, jnp.int32)
        return jnp.take_along_axis(value, index, axis=1, mode="promise_in_bounds")

    for mz in range(H):
        for my in range(H):
            scl[mz, my] = pick(inverse, c * A * A + dest(z, c, False, mz) * A + dest(y, c, False, my))
    stp_s[...] = pick(step, c * A * A + z * A + y)

    def sum_send(mz, my):
        dev = (dest(z, c, False, mz), dest(y, c, False, my), c, x)
        return rdma(sums.at[mz, my], rc.at[mz, my], s1.at[mz, my], r1.at[mz, my], dev)

    for mz in range(H - 1, -1, -1):
        for j in range(7):
            rdma(rp.at[j, mz], rp.at[j, mz], sraw.at[0], rr.at[j, mz], partner).wait_recv()

        def one(i, carry):
            my = H - 1 - i
            zp, yp = dest(z, c, False, mz), dest(y, c, False, my)
            scale = scl[mz, my]
            for t in range(TILES):
                cols = pl.ds(t * 128, 128)

                def rounded(tile, j):
                    whole = jnp.floor(tile.astype(jnp.float32) * scale).astype(jnp.int32)
                    return (whole + noise[j, mz, my, :, cols]) >> 20

                both = rounded(gv[c, zp, yp, :, cols], 7)
                for j in range(7):
                    both += rounded(rp[j, mz, my, :, cols], j)
                sums[mz, my, :, cols] = both.astype(jnp.int16)
            if mz:
                sum_send(mz, my).start()
            else:

                @pl.when(my > 0)
                def _():
                    sum_send(mz, my).start()

            return carry

        lax.fori_loop(0, H, one, 0)

    def gather(i, total):
        mz, my = i >> 2, i & 3
        sum_send(mz, my).wait_recv()
        return total + rc[mz, my].astype(jnp.int32)

    total = lax.fori_loop(1, H * H, gather, sums[0, 0].astype(jnp.int32)).astype(jnp.float32)
    own = stp_s[...]
    share = own * (1.0 / (2 * A * A))
    for t in range(TILES):
        rx[x, :, t * 128 : (t + 1) * 128] = total[:, t * 128 : (t + 1) * 128] * share
    rx[x, :, COLS:] = own

    def send_x(k, carry):
        xp = (x + k) & 3
        rdma(rx.at[x], rx.at[x], sx.at[xp], rxs.at[x], (z, y, c, xp)).start()
        return carry

    lax.fori_loop(1, X, send_x, 0)

    for i in range(7):
        rdma(offv, roff.at[i], so.at[i], ro.at[i], partner).wait_send()
        rdma(rp.at[i], rp.at[i], sraw.at[i], rr.at[i, 0], partner).wait_send()

    def drain15(i, carry):
        sum_send(i >> 2, i & 3).wait_send()
        return carry

    lax.fori_loop(1, H * H, drain15, 0)

    def drain16(k, carry):
        p = (me16 + k) & 15
        rdma(mxs, rm1.at[me16], sm1.at[p], sr1.at[me16], partner).wait_send()
        return carry

    lax.fori_loop(1, 2 * A, drain16, 0)

    def drain8(k, carry):
        rdma(mxs2, rm2.at[z], sm2.at[(z + k) & 7], sr2.at[z], partner).wait_send()
        return carry

    lax.fori_loop(1, A, drain8, 0)

    def wait_x(k, carry):
        xp = (x + k) & 3
        rdma(rx.at[xp], rx.at[xp], sx.at[xp], rxs.at[xp], partner).wait_recv()
        return carry

    lax.fori_loop(1, X, wait_x, 0)

    def drain4(k, carry):
        xp = (x + k) & 3
        rdma(rx.at[x], rx.at[x], sx.at[xp], rxs.at[x], partner).wait_send()
        return carry

    lax.fori_loop(1, X, drain4, 0)


def finish(rx, se_ref, mw_ref, mean_o, new_o, step_o):
    x = lax.axis_index("expert")
    value = rx[X - 1]
    for s in range(X - 1):
        value = jnp.where(se_ref[s] == x, rx[s], value)
    mean = value[:, :COLS]
    mean_o[...] = mean
    new_o[...] = mw_ref[...] - learn_rate * mean
    step_o[...] = value[0:1, COLS : COLS + 1]


def body(expert_grads, round_offsets, slot_expert, master_weight):
    f32, bf16, i32 = jnp.float32, jnp.bfloat16, jnp.int32
    dma = pltpu.SemaphoreType.DMA
    vmem = pl.BlockSpec(memory_space=pltpu.VMEM)
    hbm = pl.BlockSpec(memory_space=pl.ANY)
    gathered = pl.pallas_call(
        kernel,
        name="average",
        out_shape=pltpu.VMEM((X, ROWS, COLS + 128), f32),
        in_specs=[hbm, hbm],
        out_specs=vmem,
        scratch_shapes=[
            pltpu.VMEM((2, A, A, ROWS, COLS), bf16),
            pltpu.VMEM((7, H, H, ROWS, COLS), bf16),
            pltpu.VMEM((A, 128), i32),
            pltpu.VMEM((7, A, 128), i32),
            pltpu.VMEM((8, 128, 128), i32),
            pltpu.VMEM((8, H, H, ROWS, COLS), i32),
            pltpu.VMEM((2 * A * A * ROWS, 128), f32),
            pltpu.VMEM((1, 128), f32),
            pltpu.VMEM((2 * A, 1, 128), f32),
            pltpu.VMEM((1, 128), f32),
            pltpu.VMEM((A, 1, 128), f32),
            pltpu.VMEM((ROWS, 128), f32),
            pltpu.VMEM((H, H, ROWS, 128), f32),
            pltpu.VMEM((H, H, ROWS, COLS), jnp.int16),
            pltpu.VMEM((H, H, ROWS, COLS), jnp.int16),
            dma((CHUNKS, 2)),
            dma((1,)),
            dma((7,)),
            dma((7,)),
            dma((7,)),
            dma((7, H)),
            dma((2 * A,)),
            dma((2 * A,)),
            dma((A,)),
            dma((A,)),
            dma((H, H)),
            dma((H, H)),
            dma((X,)),
            dma((X,)),
        ],
        compiler_params=pltpu.CompilerParams(collective_id=0, has_side_effects=True),
    )(expert_grads.reshape(A, A, 2, ROWS, COLS), round_offsets.reshape(A, 128))
    mean, new, step = pl.pallas_call(
        finish,
        name="finish",
        out_shape=(
            jax.ShapeDtypeStruct((ROWS, COLS), f32),
            jax.ShapeDtypeStruct((ROWS, COLS), f32),
            jax.ShapeDtypeStruct((1, 1), f32),
        ),
        in_specs=[vmem, pl.BlockSpec(memory_space=pltpu.SMEM), vmem],
        out_specs=(vmem, vmem, vmem),
        compiler_params=pltpu.CompilerParams(vmem_limit_bytes=1024 * 1024),
    )(gathered, slot_expert, master_weight.reshape(ROWS, COLS))
    return mean[None], new[None], step


def solution(mesh):
    finer = Mesh(
        mesh.devices.reshape(A, A, 2, mesh.shape["expert"]), ("dp_0", "dp_1", "dp_2", "expert")
    )
    return jax.shard_map(
        body,
        mesh=finer,
        in_specs=(P(DP, "expert", None, None), P(DP, "expert", None), P(), P("expert", DP, None)),
        out_specs=(P("expert", DP, None), P("expert", DP, None), P("expert", DP)),
        check_vma=False,
    )
```

```python
import jax
import jax.numpy as jnp
from jax import lax
from jax.experimental import pallas as pl
from jax.experimental.pallas import tpu as pltpu
from jax.sharding import Mesh
from jax.sharding import PartitionSpec as P

DP = ("dp_0", "dp_1", "dp_2")
MESH = pl.DeviceIdType.MESH
A = 8
X = 4
H = A // 2
ROWS = 8
COLS = 896
TILES = COLS // 128
CHUNKS = 4
low_power = -30
high_power = 30
learn_rate = 0.05
HASH_MUL = 747796405
HASH_ADD = 1013904223
HASH_MIX = 1103515245


def plan():
    tasks = []
    for mz in range(H):
        for my in range(H):
            along_y = mz + my > 1 or my > mz
            along_z = mz + my > 1 or mz > my
            for fz in (mz,) if along_z else (mz, -1 - mz):
                for fy in (my,) if along_y else (my, -1 - my):
                    tasks.append((fz, fy, along_y, along_z))

    def hops(task):
        return sum(f if f >= 0 else -f for f in task[:2])

    return sorted(tasks, key=lambda task: (-hops(task), task))


TASKS = plan()
N = len(TASKS)
OF = [
    list(range(N)),
    [i for i in range(N) if TASKS[i][2]],
    [i for i in range(N) if TASKS[i][3]],
    [i for i in range(N) if TASKS[i][2] and TASKS[i][3]],
]
WAVES = [range(N * w // 4, N * (w + 1) // 4) for w in range(4)]
SIZES = [len(OF[q]) for q in (0, 1, 1, 2, 2, 3, 3, 0)]
BASE = [sum(SIZES[:j]) for j in range(8)]
FIRST = (0.5, 1.0, 0.4, 1.0)
SENDS = [
    [(q, i) for i in range(N) for q in (3, 1, 2, 0) if i in OF[q] and (OF[q].index(i) < FIRST[q] * len(OF[q])) == early]
    for early in (True, False)
]


def kernel(
    g_hbm, off_hbm, rx,
    gv, rp0, rp1, rp2, rp3, offv, roff, toff, codes, noise, pm, mxs, rm1, mxs2, rm2, stp_s, scl, sums, rc,
    ld, lo, so, ro, sraw, rr, sm1, sr1, sm2, sr2, s1, r1, sx, rxs,
):
    z, y, c, x = (lax.axis_index(n) for n in ("dp_0", "dp_1", "dp_2", "expert"))

    def rdma(src, dst, send, recv, dev):
        return pltpu.make_async_remote_copy(
            src_ref=src, dst_ref=dst, send_sem=send, recv_sem=recv, device_id=dev, device_id_type=MESH
        )

    partner = (z, y, 1 - c, x)
    per = A // CHUNKS

    def way(position, core):
        return 2 * ((position + core) & 1) - 1

    def load(q, h):
        rows = pl.ds(q * per, per)
        return pltpu.make_async_copy(g_hbm.at[rows, :, h], gv.at[h, rows], ld.at[q, h])

    load_off = pltpu.make_async_copy(off_hbm, offv, lo.at[0])
    load_off.start()
    for q in range(CHUNKS):
        for h in range(2):
            load(q, h).start()

    barrier = pltpu.get_barrier_semaphore()
    me16 = y * 2 + c
    mz16 = z * 2 + c

    def greet(dev):
        pl.semaphore_signal(barrier, inc=1, device_id=dev, device_id_type=MESH)

    def greet16(k, carry):
        p = (me16 + k) & 15
        greet((z, p >> 1, p & 1, x))
        return carry

    def greet14(k, carry):
        p = (mz16 + k) & 15

        @pl.when((p >> 1) != z)
        def _():
            greet((p >> 1, y, p & 1, x))

        return carry

    def greet4(k, carry):
        greet((z, y, c, (x + k) & 3))
        return carry

    def near(position, core):
        return (position - way(position, core)) & 7

    lax.fori_loop(1, 2 * A, greet16, 0)
    lax.fori_loop(1, 2 * A, greet14, 0)
    lax.fori_loop(1, X, greet4, 0)
    greet((near(z, c), near(y, c), c, x))
    greet((near(z, c), near(y, c), 1 - c, x))
    greet((near(z, 1 - c), near(y, 1 - c), 1 - c, x))

    for q in range(CHUNKS):
        for h in range(2):
            load(q, h).wait()

            def block_max(i, carry):
                v = jnp.abs(gv[h, i >> 3, i & 7].astype(jnp.float32))
                m = v[:, :128]
                for t in range(1, TILES):
                    m = jnp.maximum(m, v[:, t * 128 : (t + 1) * 128])
                pm[pl.ds((h * A * A + i) * ROWS, ROWS), :] = m
                return carry

            lax.fori_loop(q * per * A, (q + 1) * per * A, block_max, 0, unroll=4)
    top = pm[pl.ds(0, 128, stride=ROWS), :]
    for r in range(1, ROWS):
        top = jnp.maximum(top, pm[pl.ds(r, 128, stride=ROWS), :])
    mine = jnp.max(top.T, axis=0, keepdims=True)
    mxs[...] = mine
    rm1[me16] = mine
    load_off.wait()

    pl.semaphore_wait(barrier, (2 * A - 1) + (2 * A - 2) + (X - 1) + 3)

    def send_max(k, carry):
        p = (y + k) & 7

        @pl.when(k + 1 - c != 0)
        def _():
            rdma(mxs, rm1.at[me16], sm1.at[p], sr1.at[me16], (z, p, 1, x)).start()

        return carry

    lax.fori_loop(0, A, send_max, 0)

    def to_near(core, q):
        return (near(z, core) if q > 1 else z, y if q == 2 else near(y, core), core, x)

    def dest(position, core, f):
        return (position + way(position, core) * f) & 7

    def spot(i, core=c, q=0):
        fz, fy = TASKS[i][:2]
        return dest(z, core, -1 - fz if q > 1 else fz), dest(y, core, -1 - fy if q in (1, 3) else fy)

    def group(q, wave):
        inside = [n for n, i in enumerate(OF[q]) if i in WAVES[wave]]
        return pl.ds(inside[0], len(inside)) if inside else None

    sources = [(0, 0)] + [(q, k) for q in (1, 2, 3) for k in range(2)]
    buffers = (rp0, rp1, rp2, rp3)

    def buffer(j):
        q, k = sources[j]
        return buffers[q] if q == 0 else buffers[q].at[k]

    rdma(offv, roff.at[0], so.at[0], ro.at[0], partner).start()
    for core in range(2):
        for q in (1, 2, 3):
            slot = 2 * q - 1 + c
            rdma(offv, roff.at[slot], so.at[3 * core + q], ro.at[slot], to_near(core, q)).start()

    def raw_send(q, i):
        wave = [w for w in range(len(WAVES)) if i in WAVES[w]][0]
        if q == 0:
            zp, yp = spot(i, 1 - c)
            rdma(gv.at[1 - c, zp, yp], rp0.at[i], sraw.at[0], rr.at[0, wave], partner).start()
            return
        n = OF[q].index(i)
        for core in range(2):
            zp, yp = spot(i, core, q)
            rdma(
                gv.at[core, zp, yp], buffers[q].at[c, n], sraw.at[3 * core + q], rr.at[2 * q - 1 + c, wave],
                to_near(core, q),
            ).start()

    for q, i in SENDS[0]:
        raw_send(q, i)

    lane = lax.broadcasted_iota(jnp.int32, (ROWS, 128), 1)
    column = [(lane + t * 128) * HASH_MUL for t in range(TILES)]

    def dither(j, value):
        start = value * HASH_MUL + HASH_ADD
        toff[...] = jnp.concatenate([start] * 16, axis=0).T
        q = 0 if j == 7 else sources[j][0]
        for n, i in enumerate(OF[q]):
            zp, yp = spot(i)
            tile = toff[pl.ds((yp * 2 + c) * ROWS, ROWS), :]
            index = jnp.full((ROWS, 128), zp, jnp.int32)
            codes[n] = jnp.take_along_axis(tile, index, axis=1, mode="promise_in_bounds")

        def one(n, carry):
            code = codes[n]
            for t in range(TILES):
                v = code + column[t]
                v = v ^ (v >> 13)
                v = v * HASH_MIX
                v = v ^ (v >> 16)
                noise[BASE[j] + n, :, pl.ds(t * 128, 128)] = v & 0xFF000
            return carry

        lax.fori_loop(0, len(OF[q]), one, 0)

    dither(7, offv[...])

    @pl.when(c == 1)
    def _():
        def wait_max(k, carry):
            p = (me16 + k) & 15
            rdma(mxs, rm1.at[p], sm1.at[0], sr1.at[p], partner).wait_recv()
            return carry

        lax.fori_loop(1, 2 * A, wait_max, 0)
        ring = jnp.max(rm1[...], axis=0)
        mxs2[...] = ring
        rm2[z] = ring

        def send_max2(k, carry):
            p = (mz16 + k) & 15
            rdma(mxs2, rm2.at[z], sm2.at[p], sr2.at[z], (p >> 1, y, p & 1, x)).start()
            return carry

        lax.fori_loop(1, 2 * A, send_max2, 0)

    for q, i in SENDS[1]:
        raw_send(q, i)
    for j in range(7):
        rdma(offv, roff.at[j], so.at[0], ro.at[j], partner).wait_recv()
        dither(j, roff[j])

    def wait_max2(k, carry):
        p = (z + k) & 7

        @pl.when(k + 1 - c != 0)
        def _():
            rdma(mxs2, rm2.at[p], sm2.at[p], sr2.at[p], partner).wait_recv()

        return carry

    lax.fori_loop(0, A, wait_max2, 0)
    best = jnp.broadcast_to(jnp.max(rm2[...], axis=0), (ROWS, 128))
    step = jnp.full((ROWS, 128), 2.0 ** (low_power - 6), jnp.float32)
    inverse = jnp.full((ROWS, 128), 2.0 ** (6 - low_power + 20), jnp.float32)
    for e in range(low_power, high_power):
        over = best >= 2.0**e
        step = jnp.where(over, jnp.float32(2.0 ** (e - 5)), step)
        inverse = jnp.where(over, jnp.float32(2.0 ** (25 - e)), inverse)

    def pick(value, block):
        index = jnp.full((ROWS, 128), block, jnp.int32)
        return jnp.take_along_axis(value, index, axis=1, mode="promise_in_bounds")

    for i in range(N):
        zp, yp = spot(i)
        scl[i] = pick(inverse, c * A * A + zp * A + yp)
    stp_s[...] = pick(step, c * A * A + z * A + y)

    def sum_send(i):
        zp, yp = spot(i)
        return rdma(sums.at[i], rc.at[i], s1.at[i], r1.at[i], (zp, yp, c, x))

    for wave in range(len(WAVES)):
        for j in range(7):
            rows = group(sources[j][0], wave)
            if rows is not None:
                rdma(buffer(j).at[rows], buffer(j).at[rows], sraw.at[0], rr.at[j, wave], partner).wait_recv()
        for i in WAVES[wave]:
            zp, yp = spot(i)
            scale = scl[i]
            parts = [(gv.at[c, zp, yp], BASE[7] + i)]
            for j in range(7):
                q = sources[j][0]
                if i in OF[q]:
                    n = OF[q].index(i)
                    parts.append((buffer(j).at[n], BASE[j] + n))

            def tile(t, carry):
                cols = pl.ds(pl.multiple_of(t * 128, 128), 128)
                both = None
                for rows, n in parts:
                    whole = jnp.floor(rows[:, cols].astype(jnp.float32) * scale).astype(jnp.int32)
                    part = (whole + noise[n, :, cols]) >> 20
                    both = part if both is None else both + part
                sums[i, :, cols] = both.astype(jnp.int16)
                return carry

            lax.fori_loop(0, TILES, tile, 0, unroll=True)
            if i < N - 1:
                sum_send(i).start()

    total = sums[N - 1].astype(jnp.int32)
    for i in range(N - 1):
        sum_send(i).wait_recv()
        total += rc[i].astype(jnp.int32)
    total = total.astype(jnp.float32)
    own = stp_s[...]
    share = own * (1.0 / (2 * A * A))
    for t in range(TILES):
        rx[x, :, t * 128 : (t + 1) * 128] = total[:, t * 128 : (t + 1) * 128] * share
    rx[x, :, COLS:] = own

    def send_x(k, carry):
        xp = (x + k) & 3
        rdma(rx.at[x], rx.at[x], sx.at[xp], rxs.at[x], (z, y, c, xp)).start()
        return carry

    lax.fori_loop(1, X, send_x, 0)

    for i in range(7):
        rdma(offv, roff.at[i], so.at[i], ro.at[i], partner).wait_send()
    for i in range(7):
        rows = buffers[(i + 2) % 3 + 1 if i else 0]
        rows = rows if i == 0 else rows.at[0]
        rdma(rows, rows, sraw.at[i], rr.at[0, 0], partner).wait_send()
    for i in range(N - 1):
        sum_send(i).wait_send()

    def drain8(k, carry):
        @pl.when(k + 1 - c != 0)
        def _():
            rdma(mxs, rm1.at[me16], sm1.at[(y + k) & 7], sr1.at[me16], partner).wait_send()

        return carry

    lax.fori_loop(0, A, drain8, 0)

    @pl.when(c == 1)
    def _():
        def drain16(k, carry):
            rdma(mxs2, rm2.at[z], sm2.at[(mz16 + k) & 15], sr2.at[z], partner).wait_send()
            return carry

        lax.fori_loop(1, 2 * A, drain16, 0)

    def wait_x(k, carry):
        xp = (x + k) & 3
        rdma(rx.at[xp], rx.at[xp], sx.at[xp], rxs.at[xp], partner).wait_recv()
        return carry

    lax.fori_loop(1, X, wait_x, 0)

    def drain4(k, carry):
        xp = (x + k) & 3
        rdma(rx.at[x], rx.at[x], sx.at[xp], rxs.at[x], partner).wait_send()
        return carry

    lax.fori_loop(1, X, drain4, 0)


def finish(rx, se_ref, mw_ref, mean_o, new_o, step_o):
    x = lax.axis_index("expert")
    value = rx[X - 1]
    for s in range(X - 1):
        value = jnp.where(se_ref[s] == x, rx[s], value)
    mean = value[:, :COLS]
    mean_o[...] = mean
    new_o[...] = mw_ref[...] - learn_rate * mean
    step_o[...] = value[0:1, COLS : COLS + 1]


def body(expert_grads, round_offsets, slot_expert, master_weight):
    f32, bf16, i32 = jnp.float32, jnp.bfloat16, jnp.int32
    dma = pltpu.SemaphoreType.DMA
    vmem = pl.BlockSpec(memory_space=pltpu.VMEM)
    hbm = pl.BlockSpec(memory_space=pl.ANY)
    gathered = pl.pallas_call(
        kernel,
        name="average",
        out_shape=pltpu.VMEM((X, ROWS, COLS + 128), f32),
        in_specs=[hbm, hbm],
        out_specs=vmem,
        scratch_shapes=[
            pltpu.VMEM((2, A, A, ROWS, COLS), bf16),
            pltpu.VMEM((N, ROWS, COLS), bf16),
            pltpu.VMEM((2, len(OF[1]), ROWS, COLS), bf16),
            pltpu.VMEM((2, len(OF[2]), ROWS, COLS), bf16),
            pltpu.VMEM((2, len(OF[3]), ROWS, COLS), bf16),
            pltpu.VMEM((A, 128), i32),
            pltpu.VMEM((7, A, 128), i32),
            pltpu.VMEM((128, 128), i32),
            pltpu.VMEM((N, ROWS, 128), i32),
            pltpu.VMEM((sum(SIZES), ROWS, COLS), i32),
            pltpu.VMEM((2 * A * A * ROWS, 128), f32),
            pltpu.VMEM((1, 128), f32),
            pltpu.VMEM((2 * A, 1, 128), f32),
            pltpu.VMEM((1, 128), f32),
            pltpu.VMEM((A, 1, 128), f32),
            pltpu.VMEM((ROWS, 128), f32),
            pltpu.VMEM((N, ROWS, 128), f32),
            pltpu.VMEM((N, ROWS, COLS), jnp.int16),
            pltpu.VMEM((N, ROWS, COLS), jnp.int16),
            dma((CHUNKS, 2)),
            dma((1,)),
            dma((7,)),
            dma((7,)),
            dma((7,)),
            dma((7, len(WAVES))),
            dma((A,)),
            dma((2 * A,)),
            dma((2 * A,)),
            dma((A,)),
            dma((N,)),
            dma((N,)),
            dma((X,)),
            dma((X,)),
        ],
        compiler_params=pltpu.CompilerParams(collective_id=0, has_side_effects=True),
    )(expert_grads.reshape(A, A, 2, ROWS, COLS), round_offsets.reshape(A, 128))
    mean, new, step = pl.pallas_call(
        finish,
        name="finish",
        out_shape=(
            jax.ShapeDtypeStruct((ROWS, COLS), f32),
            jax.ShapeDtypeStruct((ROWS, COLS), f32),
            jax.ShapeDtypeStruct((1, 1), f32),
        ),
        in_specs=[vmem, pl.BlockSpec(memory_space=pltpu.SMEM), vmem],
        out_specs=(vmem, vmem, vmem),
        compiler_params=pltpu.CompilerParams(vmem_limit_bytes=1024 * 1024),
    )(gathered, slot_expert, master_weight.reshape(ROWS, COLS))
    return mean[None], new[None], step


def solution(mesh):
    finer = Mesh(
        mesh.devices.reshape(A, A, 2, mesh.shape["expert"]), ("dp_0", "dp_1", "dp_2", "expert")
    )
    return jax.shard_map(
        body,
        mesh=finer,
        in_specs=(P(DP, "expert", None, None), P(DP, "expert", None), P(), P("expert", DP, None)),
        out_specs=(P("expert", DP, None), P("expert", DP, None), P("expert", DP)),
        check_vma=False,
    )
```

```python
import jax
import jax.numpy as jnp
from jax import lax
from jax.experimental import pallas as pl
from jax.experimental.pallas import tpu as pltpu
from jax.sharding import Mesh
from jax.sharding import PartitionSpec as P

DP = ("dp_0", "dp_1", "dp_2")
MESH = pl.DeviceIdType.MESH
A = 8
X = 4
H = A // 2
ROWS = 8
COLS = 896
TILES = COLS // 128
CHUNKS = 4
low_power = -30
high_power = 30
learn_rate = 0.05
HASH_MUL = 747796405
HASH_ADD = 1013904223
HASH_MIX = 1103515245


def plan():
    tasks = []
    for mz in range(H):
        for my in range(H):
            along_y = mz + my > 1 or my > mz
            along_z = mz + my > 1 or mz > my
            for fz in (mz,) if along_z else (mz, -1 - mz):
                for fy in (my,) if along_y else (my, -1 - my):
                    tasks.append((fz, fy, along_y, along_z))

    def hops(task):
        return sum(f if f >= 0 else -f for f in task[:2])

    return sorted(tasks, key=lambda task: (-hops(task), task))


TASKS = plan()
N = len(TASKS)
OF = [
    list(range(N)),
    [i for i in range(N) if TASKS[i][2]],
    [i for i in range(N) if TASKS[i][3]],
    [i for i in range(N) if TASKS[i][2] and TASKS[i][3]],
]
WAVES = [range(N * w // 4, N * (w + 1) // 4) for w in range(4)]
SIZES = [len(OF[q]) for q in (0, 1, 1, 2, 2, 3, 3, 0)]
BASE = [sum(SIZES[:j]) for j in range(8)]
FIRST = (0.5, 1.0, 0.4, 1.0)
SENDS = [
    [(q, i) for i in range(N) for q in (3, 1, 2, 0) if i in OF[q] and (OF[q].index(i) < FIRST[q] * len(OF[q])) == early]
    for early in (True, False)
]


def kernel(
    g_hbm, off_hbm, rx,
    gv, rp, offv, roff, toff, codes, noise, pm, mxs, rm1, mxs2, rm2, stp_s, scl, sums, rc,
    ld, lo, so, ro, sraw, rr, sm1, sr1, sm2, sr2, s1, r1, sx, rxs,
):
    z, y, c, x = (lax.axis_index(n) for n in ("dp_0", "dp_1", "dp_2", "expert"))

    def rdma(src, dst, send, recv, dev):
        return pltpu.make_async_remote_copy(
            src_ref=src, dst_ref=dst, send_sem=send, recv_sem=recv, device_id=dev, device_id_type=MESH
        )

    partner = (z, y, 1 - c, x)
    per = A // CHUNKS

    def way(position, core):
        return 2 * ((position + core) & 1) - 1

    def load(q, h):
        rows = pl.ds(q * per, per)
        return pltpu.make_async_copy(g_hbm.at[rows, :, h], gv.at[h, rows], ld.at[q, h])

    load_off = pltpu.make_async_copy(off_hbm, offv, lo.at[0])
    load_off.start()
    for q in range(CHUNKS):
        for h in range(2):
            load(q, h).start()

    barrier = pltpu.get_barrier_semaphore()
    me16 = y * 2 + c
    mz16 = z * 2 + c

    def greet(dev):
        pl.semaphore_signal(barrier, inc=1, device_id=dev, device_id_type=MESH)

    def greet16(k, carry):
        p = (me16 + k) & 15
        greet((z, p >> 1, p & 1, x))
        return carry

    def greet14(k, carry):
        p = (mz16 + k) & 15

        @pl.when((p >> 1) != z)
        def _():
            greet((p >> 1, y, p & 1, x))

        return carry

    def greet4(k, carry):
        greet((z, y, c, (x + k) & 3))
        return carry

    def near(position, core):
        return (position - way(position, core)) & 7

    lax.fori_loop(1, 2 * A, greet16, 0)
    lax.fori_loop(1, 2 * A, greet14, 0)
    lax.fori_loop(1, X, greet4, 0)
    greet((near(z, c), near(y, c), c, x))
    greet((near(z, c), near(y, c), 1 - c, x))
    greet((near(z, 1 - c), near(y, 1 - c), 1 - c, x))

    for q in range(CHUNKS):
        for h in range(2):
            load(q, h).wait()

            def block_max(i, carry):
                v = jnp.abs(gv[h, i >> 3, i & 7].astype(jnp.float32))
                m = v[:, :128]
                for t in range(1, TILES):
                    m = jnp.maximum(m, v[:, t * 128 : (t + 1) * 128])
                pm[pl.ds((h * A * A + i) * ROWS, ROWS), :] = m
                return carry

            lax.fori_loop(q * per * A, (q + 1) * per * A, block_max, 0, unroll=4)
    top = pm[pl.ds(0, 128, stride=ROWS), :]
    for r in range(1, ROWS):
        top = jnp.maximum(top, pm[pl.ds(r, 128, stride=ROWS), :])
    mine = jnp.max(top.T, axis=0, keepdims=True)
    mxs[...] = mine
    rm1[me16] = mine
    load_off.wait()

    pl.semaphore_wait(barrier, (2 * A - 1) + (2 * A - 2) + (X - 1) + 3)

    def send_max(k, carry):
        p = (y + k) & 7

        @pl.when(k + 1 - c != 0)
        def _():
            rdma(mxs, rm1.at[me16], sm1.at[0], sr1.at[0], (z, p, 1, x)).start()

        return carry

    lax.fori_loop(0, A, send_max, 0)

    def to_near(core, q):
        return (near(z, core) if q > 1 else z, y if q == 2 else near(y, core), core, x)

    def dest(position, core, f):
        return (position + way(position, core) * f) & 7

    def spot(i, core=c, q=0):
        fz, fy = TASKS[i][:2]
        return dest(z, core, -1 - fz if q > 1 else fz), dest(y, core, -1 - fy if q in (1, 3) else fy)

    sources = [(0, 0)] + [(q, k) for q in (1, 2, 3) for k in range(2)]

    rdma(offv, roff.at[0], so.at[0], ro.at[0], partner).start()
    for core in range(2):
        for q in (1, 2, 3):
            slot = 2 * q - 1 + c
            rdma(offv, roff.at[slot], so.at[3 * core + q], ro.at[slot], to_near(core, q)).start()

    def raw_send(q, i):
        wave = [w for w in range(len(WAVES)) if i in WAVES[w]][0]
        if q == 0:
            zp, yp = spot(i, 1 - c)
            rdma(gv.at[1 - c, zp, yp], rp.at[i], sraw.at[0], rr.at[wave], partner).start()
            return
        n = OF[q].index(i)
        for core in range(2):
            zp, yp = spot(i, core, q)
            rdma(
                gv.at[core, zp, yp], rp.at[BASE[2 * q - 1] + c * len(OF[q]) + n], sraw.at[0], rr.at[wave], to_near(core, q)
            ).start()

    for q, i in SENDS[0]:
        raw_send(q, i)

    lane = lax.broadcasted_iota(jnp.int32, (ROWS, 128), 1)
    column = [(lane + t * 128) * HASH_MUL for t in range(TILES)]

    def dither(j, value):
        start = value * HASH_MUL + HASH_ADD
        toff[...] = jnp.concatenate([start] * 16, axis=0).T
        q = 0 if j == 7 else sources[j][0]
        for n, i in enumerate(OF[q]):
            zp, yp = spot(i)
            tile = toff[pl.ds((yp * 2 + c) * ROWS, ROWS), :]
            index = jnp.full((ROWS, 128), zp, jnp.int32)
            codes[n] = jnp.take_along_axis(tile, index, axis=1, mode="promise_in_bounds")

        def one(n, carry):
            code = codes[n]
            for t in range(TILES):
                v = code + column[t]
                v = v ^ (v >> 13)
                v = v * HASH_MIX
                v = v ^ (v >> 16)
                noise[BASE[j] + n, :, pl.ds(t * 128, 128)] = v & 0xFF000
            return carry

        lax.fori_loop(0, len(OF[q]), one, 0)

    dither(7, offv[...])

    @pl.when(c == 1)
    def _():
        others = rm1.at[pl.ds(0, 2 * A - 1)]
        rdma(others, others, sm1.at[0], sr1.at[0], partner).wait_recv()
        ring = jnp.max(rm1[...], axis=0)
        mxs2[...] = ring
        rm2[z] = ring

        def send_max2(k, carry):
            p = (mz16 + k) & 15
            rdma(mxs2, rm2.at[z], sm2.at[0], sr2.at[0], (p >> 1, y, p & 1, x)).start()
            return carry

        lax.fori_loop(1, 2 * A, send_max2, 0)

    for q, i in SENDS[1]:
        raw_send(q, i)
    for j in range(7):
        rdma(offv, roff.at[j], so.at[0], ro.at[j], partner).wait_recv()
        dither(j, roff[j])

    for core in range(2):

        @pl.when(c == core)
        def _():
            others = rm2.at[pl.ds(0, A - core)]
            rdma(others, others, sm2.at[0], sr2.at[0], partner).wait_recv()

    best = jnp.broadcast_to(jnp.max(rm2[...], axis=0), (ROWS, 128))
    step = jnp.full((ROWS, 128), 2.0 ** (low_power - 6), jnp.float32)
    inverse = jnp.full((ROWS, 128), 2.0 ** (6 - low_power + 20), jnp.float32)
    for e in range(low_power, high_power):
        over = best >= 2.0**e
        step = jnp.where(over, jnp.float32(2.0 ** (e - 5)), step)
        inverse = jnp.where(over, jnp.float32(2.0 ** (25 - e)), inverse)

    def pick(value, block):
        index = jnp.full((ROWS, 128), block, jnp.int32)
        return jnp.take_along_axis(value, index, axis=1, mode="promise_in_bounds")

    for i in range(N):
        zp, yp = spot(i)
        scl[i] = pick(inverse, c * A * A + zp * A + yp)
    stp_s[...] = pick(step, c * A * A + z * A + y)

    def sum_send(i):
        zp, yp = spot(i)
        return rdma(sums.at[i], rc.at[i], s1.at[0], r1.at[0 if i < N // 2 else 1], (zp, yp, c, x))

    for wave in range(len(WAVES)):
        arrived = rp.at[pl.ds(0, sum(i in WAVES[wave] for q, _ in sources for i in OF[q]))]
        rdma(arrived, arrived, sraw.at[0], rr.at[wave], partner).wait_recv()
        for i in WAVES[wave]:
            zp, yp = spot(i)
            scale = scl[i]
            parts = [(gv.at[c, zp, yp], BASE[7] + i)]
            for j in range(7):
                q = sources[j][0]
                if i in OF[q]:
                    n = OF[q].index(i)
                    parts.append((rp.at[BASE[j] + n], BASE[j] + n))

            def tile(t, carry):
                cols = pl.ds(pl.multiple_of(t * 128, 128), 128)
                both = None
                for rows, n in parts:
                    whole = jnp.floor(rows[:, cols].astype(jnp.float32) * scale).astype(jnp.int32)
                    part = (whole + noise[n, :, cols]) >> 20
                    both = part if both is None else both + part
                sums[i, :, cols] = both.astype(jnp.int16)
                return carry

            lax.fori_loop(0, TILES, tile, 0, unroll=True)
            if i < N - 1:
                sum_send(i).start()

    total = sums[N - 1].astype(jnp.int32)
    for part, rows in enumerate((range(N // 2), range(N // 2, N - 1))):
        half = rc.at[pl.ds(rows[0], len(rows))]
        rdma(half, half, s1.at[0], r1.at[part], partner).wait_recv()
        for i in rows:
            total += rc[i].astype(jnp.int32)
    total = total.astype(jnp.float32)
    own = stp_s[...]
    share = own * (1.0 / (2 * A * A))
    for t in range(TILES):
        rx[x, :, t * 128 : (t + 1) * 128] = total[:, t * 128 : (t + 1) * 128] * share
    rx[x, :, COLS:] = own

    def send_x(k, carry):
        xp = (x + k) & 3
        rdma(rx.at[x], rx.at[x], sx.at[0], rxs.at[0], (z, y, c, xp)).start()
        return carry

    for k in (2, 1, 3):
        send_x(k, 0)

    for i in range(7):
        rdma(offv, roff.at[i], so.at[i], ro.at[i], partner).wait_send()
    rdma(rp, rp, sraw.at[0], rr.at[0], partner).wait_send()
    rdma(rc.at[pl.ds(0, N - 1)], rc.at[pl.ds(0, N - 1)], s1.at[0], r1.at[0], partner).wait_send()

    for core in range(2):

        @pl.when(c == core)
        def _():
            others = rm2.at[pl.ds(0, A - core)]
            rdma(others, others, sm1.at[0], sr2.at[0], partner).wait_send()
            if core:
                others = rm1.at[pl.ds(0, 2 * A - 1)]
                rdma(others, others, sm2.at[0], sr1.at[0], partner).wait_send()

    others = rx.at[pl.ds(0, X - 1)]
    rdma(others, others, sx.at[0], rxs.at[0], partner).wait_recv()
    rdma(others, others, sx.at[0], rxs.at[0], partner).wait_send()


def finish(rx, se_ref, mw_ref, mean_o, new_o, step_o):
    x = lax.axis_index("expert")
    value = rx[X - 1]
    for s in range(X - 1):
        value = jnp.where(se_ref[:, s : s + 1] == x, rx[s], value)
    mean = value[:, :COLS]
    mean_o[...] = mean
    new_o[...] = mw_ref[...] - learn_rate * mean
    step_o[...] = value[0:1, COLS : COLS + 1]


def body(expert_grads, round_offsets, slot_expert, master_weight):
    f32, bf16, i32 = jnp.float32, jnp.bfloat16, jnp.int32
    dma = pltpu.SemaphoreType.DMA
    vmem = pl.BlockSpec(memory_space=pltpu.VMEM)
    hbm = pl.BlockSpec(memory_space=pl.ANY)
    gathered = pl.pallas_call(
        kernel,
        name="average",
        out_shape=pltpu.VMEM((X, ROWS, COLS + 128), f32),
        in_specs=[hbm, hbm],
        out_specs=vmem,
        scratch_shapes=[
            pltpu.VMEM((2, A, A, ROWS, COLS), bf16),
            pltpu.VMEM((BASE[7], ROWS, COLS), bf16),
            pltpu.VMEM((A, 128), i32),
            pltpu.VMEM((7, A, 128), i32),
            pltpu.VMEM((128, 128), i32),
            pltpu.VMEM((N, ROWS, 128), i32),
            pltpu.VMEM((sum(SIZES), ROWS, COLS), i32),
            pltpu.VMEM((2 * A * A * ROWS, 128), f32),
            pltpu.VMEM((1, 128), f32),
            pltpu.VMEM((2 * A, 1, 128), f32),
            pltpu.VMEM((1, 128), f32),
            pltpu.VMEM((A, 1, 128), f32),
            pltpu.VMEM((ROWS, 128), f32),
            pltpu.VMEM((N, ROWS, 128), f32),
            pltpu.VMEM((N, ROWS, COLS), jnp.int16),
            pltpu.VMEM((N, ROWS, COLS), jnp.int16),
            dma((CHUNKS, 2)),
            dma((1,)),
            dma((7,)),
            dma((7,)),
            dma((1,)),
            dma((len(WAVES),)),
            dma((1,)),
            dma((1,)),
            dma((1,)),
            dma((1,)),
            dma((1,)),
            dma((2,)),
            dma((1,)),
            dma((1,)),
        ],
        compiler_params=pltpu.CompilerParams(collective_id=0, has_side_effects=True),
    )(expert_grads.reshape(A, A, 2, ROWS, COLS), round_offsets.reshape(A, 128))
    mean, new, step = pl.pallas_call(
        finish,
        name="finish",
        out_shape=(
            jax.ShapeDtypeStruct((ROWS, COLS), f32),
            jax.ShapeDtypeStruct((ROWS, COLS), f32),
            jax.ShapeDtypeStruct((1, 1), f32),
        ),
        in_specs=[vmem, vmem, vmem],
        out_specs=(vmem, vmem, vmem),
        compiler_params=pltpu.CompilerParams(vmem_limit_bytes=1024 * 1024),
    )(gathered, slot_expert.reshape(1, X), master_weight.reshape(ROWS, COLS))
    return mean[None], new[None], step


def solution(mesh):
    finer = Mesh(
        mesh.devices.reshape(A, A, 2, mesh.shape["expert"]), ("dp_0", "dp_1", "dp_2", "expert")
    )
    return jax.shard_map(
        body,
        mesh=finer,
        in_specs=(P(DP, "expert", None, None), P(DP, "expert", None), P(), P("expert", DP, None)),
        out_specs=(P("expert", DP, None), P("expert", DP, None), P("expert", DP)),
        check_vma=False,
    )
```

```python
import jax
import jax.numpy as jnp
from jax import lax
from jax.experimental import pallas as pl
from jax.experimental.pallas import tpu as pltpu
from jax.sharding import Mesh
from jax.sharding import PartitionSpec as P

DP = ("dp_0", "dp_1", "dp_2")
MESH = pl.DeviceIdType.MESH
A = 8
X = 4
H = A // 2
ROWS = 8
COLS = 896
TILES = COLS // 128
CHUNKS = 4
low_power = -30
high_power = 30
learn_rate = 0.05
HASH_MUL = 747796405
HASH_ADD = 1013904223
HASH_MIX = 1103515245


def plan():
    tasks = []
    for mz in range(H):
        for my in range(H):
            along_y = mz + my > 1 or my > mz
            along_z = mz + my > 1 or mz > my
            for fz in (mz,) if along_z else (mz, -1 - mz):
                for fy in (my,) if along_y else (my, -1 - my):
                    tasks.append((fz, fy, along_y, along_z))

    def hops(task):
        return sum(f if f >= 0 else -f for f in task[:2])

    return sorted(tasks, key=lambda task: (-hops(task), task))


TASKS = plan()
N = len(TASKS)
OF = [
    list(range(N)),
    [i for i in range(N) if TASKS[i][2]],
    [i for i in range(N) if TASKS[i][3]],
    [i for i in range(N) if TASKS[i][2] and TASKS[i][3]],
]
WAVES = [range(N * w // 4, N * (w + 1) // 4) for w in range(4)]
SIZES = [len(OF[q]) for q in (0, 1, 1, 2, 2, 3, 3, 0)]
BASE = [sum(SIZES[:j]) for j in range(8)]
FIRST = (0.5, 1.0, 0.4, 1.0)
SENDS = [
    [(q, i) for i in range(N) for q in (3, 1, 2, 0) if i in OF[q] and (OF[q].index(i) < FIRST[q] * len(OF[q])) == early]
    for early in (True, False)
]


def kernel(
    g_hbm, off_hbm, rx,
    gv, rp, offv, roff, toff, codes, noise, pm, mxs, rm1, mxs2, rm2, stp_s, scl, sums, rc,
    ld, lo, so, ro, sraw, rr, sm1, sr1, sm2, sr2, s1, r1, sx, rxs,
):
    z, y, c, x = (lax.axis_index(n) for n in ("dp_0", "dp_1", "dp_2", "expert"))

    def rdma(src, dst, send, recv, dev):
        return pltpu.make_async_remote_copy(
            src_ref=src, dst_ref=dst, send_sem=send, recv_sem=recv, device_id=dev, device_id_type=MESH
        )

    partner = (z, y, 1 - c, x)
    per = A // CHUNKS

    def way(position, core):
        return 2 * ((position + core) & 1) - 1

    def load(q, h):
        rows = pl.ds(q * per, per)
        return pltpu.make_async_copy(g_hbm.at[rows, :, h], gv.at[h, rows], ld.at[q, h])

    load_off = pltpu.make_async_copy(off_hbm, offv, lo.at[0])
    load_off.start()
    for q in range(CHUNKS):
        for h in range(2):
            load(q, h).start()

    barrier = pltpu.get_barrier_semaphore()
    me16 = y * 2 + c
    mz16 = z * 2 + c

    def greet(dev):
        pl.semaphore_signal(barrier, inc=1, device_id=dev, device_id_type=MESH)

    def greet16(k, carry):
        p = (me16 + k) & 15
        greet((z, p >> 1, p & 1, x))
        return carry

    def greet14(k, carry):
        p = (mz16 + k) & 15

        @pl.when((p >> 1) != z)
        def _():
            greet((p >> 1, y, p & 1, x))

        return carry

    def greet4(k, carry):
        greet((z, y, c, (x + k) & 3))
        return carry

    def near(position, core):
        return (position - way(position, core)) & 7

    far = sorted(range(1, 2 * A), key=lambda k: -min(k, 2 * A - k))
    for k in far:
        greet14(k, 0)
        greet16(k, 0)
    lax.fori_loop(1, X, greet4, 0)
    greet((near(z, c), near(y, c), c, x))
    greet((near(z, c), near(y, c), 1 - c, x))
    greet((near(z, 1 - c), near(y, 1 - c), 1 - c, x))

    for q in range(CHUNKS):
        for h in range(2):
            load(q, h).wait()

            def block_max(i, carry):
                v = jnp.abs(gv[h, i >> 3, i & 7].astype(jnp.float32))
                m = v[:, :128]
                for t in range(1, TILES):
                    m = jnp.maximum(m, v[:, t * 128 : (t + 1) * 128])
                pm[pl.ds((h * A * A + i) * ROWS, ROWS), :] = m
                return carry

            lax.fori_loop(q * per * A, (q + 1) * per * A, block_max, 0, unroll=4)
    top = pm[pl.ds(0, 128, stride=ROWS), :]
    for r in range(1, ROWS):
        top = jnp.maximum(top, pm[pl.ds(r, 128, stride=ROWS), :])
    mine = jnp.max(top.T, axis=0, keepdims=True)
    mxs[...] = mine
    rm1[me16] = mine
    load_off.wait()

    pl.semaphore_wait(barrier, (2 * A - 1) + (2 * A - 2) + (X - 1) + 3)

    def send_max(k, carry):
        p = (y + k) & 7

        @pl.when(k + 1 - c != 0)
        def _():
            rdma(mxs, rm1.at[me16], sm1.at[0], sr1.at[0], (z, p, 1, x)).start()

        return carry

    lax.fori_loop(0, A, send_max, 0)

    def to_near(core, q):
        return (near(z, core) if q > 1 else z, y if q == 2 else near(y, core), core, x)

    def dest(position, core, f):
        return (position + way(position, core) * f) & 7

    def spot(i, core=c, q=0):
        fz, fy = TASKS[i][:2]
        return dest(z, core, -1 - fz if q > 1 else fz), dest(y, core, -1 - fy if q in (1, 3) else fy)

    sources = [(0, 0)] + [(q, k) for q in (1, 2, 3) for k in range(2)]

    rdma(offv, roff.at[0], so.at[0], ro.at[0], partner).start()
    for core in range(2):
        for q in (1, 2, 3):
            slot = 2 * q - 1 + c
            rdma(offv, roff.at[slot], so.at[3 * core + q], ro.at[slot], to_near(core, q)).start()

    def raw_send(q, i):
        wave = [w for w in range(len(WAVES)) if i in WAVES[w]][0]
        if q == 0:
            zp, yp = spot(i, 1 - c)
            rdma(gv.at[1 - c, zp, yp], rp.at[i], sraw.at[0], rr.at[wave], partner).start()
            return
        n = OF[q].index(i)
        for core in range(2):
            zp, yp = spot(i, core, q)
            rdma(
                gv.at[core, zp, yp], rp.at[BASE[2 * q - 1] + c * len(OF[q]) + n], sraw.at[0], rr.at[wave], to_near(core, q)
            ).start()

    for q, i in SENDS[0]:
        raw_send(q, i)

    lane = lax.broadcasted_iota(jnp.int32, (ROWS, 128), 1)
    column = [(lane + t * 128) * HASH_MUL for t in range(TILES)]

    def dither(j, value):
        start = value * HASH_MUL + HASH_ADD
        toff[...] = jnp.concatenate([start] * 16, axis=0).T
        q = 0 if j == 7 else sources[j][0]
        for n, i in enumerate(OF[q]):
            zp, yp = spot(i)
            tile = toff[pl.ds((yp * 2 + c) * ROWS, ROWS), :]
            index = jnp.full((ROWS, 128), zp, jnp.int32)
            codes[n] = jnp.take_along_axis(tile, index, axis=1, mode="promise_in_bounds")

        def one(n, carry):
            code = codes[n]
            for t in range(TILES):
                v = code + column[t]
                v = v ^ (v >> 13)
                v = v * HASH_MIX
                v = v ^ (v >> 16)
                noise[BASE[j] + n, :, pl.ds(t * 128, 128)] = v & 0xFF000
            return carry

        lax.fori_loop(0, len(OF[q]), one, 0)

    dither(7, offv[...])

    @pl.when(c == 1)
    def _():
        others = rm1.at[pl.ds(0, 2 * A - 1)]
        rdma(others, others, sm1.at[0], sr1.at[0], partner).wait_recv()
        ring = jnp.max(rm1[...], axis=0)
        mxs2[...] = ring
        rm2[z] = ring

        def send_max2(k, carry):
            p = (mz16 + k) & 15
            rdma(mxs2, rm2.at[z], sm2.at[0], sr2.at[0], (p >> 1, y, p & 1, x)).start()
            return carry

        lax.fori_loop(1, 2 * A, send_max2, 0)

    for q, i in SENDS[1]:
        raw_send(q, i)
    for j in range(7):
        rdma(offv, roff.at[j], so.at[0], ro.at[j], partner).wait_recv()
        dither(j, roff[j])

    for core in range(2):

        @pl.when(c == core)
        def _():
            others = rm2.at[pl.ds(0, A - core)]
            rdma(others, others, sm2.at[0], sr2.at[0], partner).wait_recv()

    best = jnp.broadcast_to(jnp.max(rm2[...], axis=0), (ROWS, 128))
    step = jnp.full((ROWS, 128), 2.0 ** (low_power - 6), jnp.float32)
    inverse = jnp.full((ROWS, 128), 2.0 ** (6 - low_power + 20), jnp.float32)
    for e in range(low_power, high_power):
        over = best >= 2.0**e
        step = jnp.where(over, jnp.float32(2.0 ** (e - 5)), step)
        inverse = jnp.where(over, jnp.float32(2.0 ** (25 - e)), inverse)

    def pick(value, block):
        index = jnp.full((ROWS, 128), block, jnp.int32)
        return jnp.take_along_axis(value, index, axis=1, mode="promise_in_bounds")

    for i in range(N):
        zp, yp = spot(i)
        scl[i] = pick(inverse, c * A * A + zp * A + yp)
    stp_s[...] = pick(step, c * A * A + z * A + y)

    def sum_send(i):
        zp, yp = spot(i)
        return rdma(sums.at[i], rc.at[i], s1.at[0], r1.at[0 if i < N // 2 else 1], (zp, yp, c, x))

    for wave in range(len(WAVES)):
        arrived = rp.at[pl.ds(0, sum(i in WAVES[wave] for q, _ in sources for i in OF[q]))]
        rdma(arrived, arrived, sraw.at[0], rr.at[wave], partner).wait_recv()
        for i in WAVES[wave]:
            zp, yp = spot(i)
            scale = scl[i]
            parts = [(gv.at[c, zp, yp], BASE[7] + i)]
            for j in range(7):
                q = sources[j][0]
                if i in OF[q]:
                    n = OF[q].index(i)
                    parts.append((rp.at[BASE[j] + n], BASE[j] + n))

            def tile(t, carry):
                cols = pl.ds(pl.multiple_of(t * 128, 128), 128)
                both = None
                for rows, n in parts:
                    whole = jnp.floor(rows[:, cols].astype(jnp.float32) * scale).astype(jnp.int32)
                    part = (whole + noise[n, :, cols]) >> 20
                    both = part if both is None else both + part
                sums[i, :, cols] = both.astype(jnp.int16)
                return carry

            lax.fori_loop(0, TILES, tile, 0, unroll=True)
            if i < N - 1:
                sum_send(i).start()

    total = sums[N - 1].astype(jnp.int32)
    for part, rows in enumerate((range(N // 2), range(N // 2, N - 1))):
        half = rc.at[pl.ds(rows[0], len(rows))]
        rdma(half, half, s1.at[0], r1.at[part], partner).wait_recv()
        for i in rows:
            total += rc[i].astype(jnp.int32)
    total = total.astype(jnp.float32)
    own = stp_s[...]
    share = own * (1.0 / (2 * A * A))
    for t in range(TILES):
        rx[x, :, t * 128 : (t + 1) * 128] = total[:, t * 128 : (t + 1) * 128] * share
    rx[x, :, COLS:] = own

    def send_x(k, carry):
        xp = (x + k) & 3
        rdma(rx.at[x], rx.at[x], sx.at[0], rxs.at[0], (z, y, c, xp)).start()
        return carry

    for k in (2, 1, 3):
        send_x(k, 0)

    for i in range(7):
        rdma(offv, roff.at[i], so.at[i], ro.at[i], partner).wait_send()
    rdma(rp, rp, sraw.at[0], rr.at[0], partner).wait_send()
    rdma(rc.at[pl.ds(0, N - 1)], rc.at[pl.ds(0, N - 1)], s1.at[0], r1.at[0], partner).wait_send()

    for core in range(2):

        @pl.when(c == core)
        def _():
            others = rm2.at[pl.ds(0, A - core)]
            rdma(others, others, sm1.at[0], sr2.at[0], partner).wait_send()
            if core:
                others = rm1.at[pl.ds(0, 2 * A - 1)]
                rdma(others, others, sm2.at[0], sr1.at[0], partner).wait_send()

    others = rx.at[pl.ds(0, X - 1)]
    rdma(others, others, sx.at[0], rxs.at[0], partner).wait_recv()
    rdma(others, others, sx.at[0], rxs.at[0], partner).wait_send()


def finish(rx, se_ref, mw_ref, mean_o, new_o, step_o):
    x = lax.axis_index("expert")
    value = rx[X - 1]
    for s in range(X - 1):
        value = jnp.where(se_ref[:, s : s + 1] == x, rx[s], value)
    mean = value[:, :COLS]
    mean_o[...] = mean
    new_o[...] = mw_ref[...] - learn_rate * mean
    step_o[...] = value[0:1, COLS : COLS + 1]


def body(expert_grads, round_offsets, slot_expert, master_weight):
    f32, bf16, i32 = jnp.float32, jnp.bfloat16, jnp.int32
    dma = pltpu.SemaphoreType.DMA
    vmem = pl.BlockSpec(memory_space=pltpu.VMEM)
    hbm = pl.BlockSpec(memory_space=pl.ANY)
    gathered = pl.pallas_call(
        kernel,
        name="average",
        out_shape=pltpu.VMEM((X, ROWS, COLS + 128), f32),
        in_specs=[hbm, hbm],
        out_specs=vmem,
        scratch_shapes=[
            pltpu.VMEM((2, A, A, ROWS, COLS), bf16),
            pltpu.VMEM((BASE[7], ROWS, COLS), bf16),
            pltpu.VMEM((A, 128), i32),
            pltpu.VMEM((7, A, 128), i32),
            pltpu.VMEM((128, 128), i32),
            pltpu.VMEM((N, ROWS, 128), i32),
            pltpu.VMEM((sum(SIZES), ROWS, COLS), i32),
            pltpu.VMEM((2 * A * A * ROWS, 128), f32),
            pltpu.VMEM((1, 128), f32),
            pltpu.VMEM((2 * A, 1, 128), f32),
            pltpu.VMEM((1, 128), f32),
            pltpu.VMEM((A, 1, 128), f32),
            pltpu.VMEM((ROWS, 128), f32),
            pltpu.VMEM((N, ROWS, 128), f32),
            pltpu.VMEM((N, ROWS, COLS), jnp.int16),
            pltpu.VMEM((N, ROWS, COLS), jnp.int16),
            dma((CHUNKS, 2)),
            dma((1,)),
            dma((7,)),
            dma((7,)),
            dma((1,)),
            dma((len(WAVES),)),
            dma((1,)),
            dma((1,)),
            dma((1,)),
            dma((1,)),
            dma((1,)),
            dma((2,)),
            dma((1,)),
            dma((1,)),
        ],
        compiler_params=pltpu.CompilerParams(collective_id=0, has_side_effects=True),
    )(expert_grads.reshape(A, A, 2, ROWS, COLS), round_offsets.reshape(A, 128))
    mean, new, step = pl.pallas_call(
        finish,
        name="finish",
        out_shape=(
            jax.ShapeDtypeStruct((ROWS, COLS), f32),
            jax.ShapeDtypeStruct((ROWS, COLS), f32),
            jax.ShapeDtypeStruct((1, 1), f32),
        ),
        in_specs=[vmem, vmem, vmem],
        out_specs=(vmem, vmem, vmem),
        compiler_params=pltpu.CompilerParams(vmem_limit_bytes=1024 * 1024),
    )(gathered, slot_expert.reshape(1, X), master_weight.reshape(ROWS, COLS))
    return mean[None], new[None], step


def solution(mesh):
    finer = Mesh(
        mesh.devices.reshape(A, A, 2, mesh.shape["expert"]), ("dp_0", "dp_1", "dp_2", "expert")
    )
    return jax.shard_map(
        body,
        mesh=finer,
        in_specs=(P(DP, "expert", None, None), P(DP, "expert", None), P(), P("expert", DP, None)),
        out_specs=(P("expert", DP, None), P("expert", DP, None), P("expert", DP)),
        check_vma=False,
    )
```

```python
import jax
import jax.numpy as jnp
from jax import lax
from jax.experimental import pallas as pl
from jax.experimental.pallas import tpu as pltpu
from jax.sharding import Mesh
from jax.sharding import PartitionSpec as P

DP = ("dp_0", "dp_1", "dp_2")
MESH = pl.DeviceIdType.MESH
A = 8
X = 4
H = A // 2
ROWS = 8
COLS = 896
TILES = COLS // 128
CHUNKS = 4
low_power = -30
high_power = 30
learn_rate = 0.05
HASH_MUL = 747796405
HASH_ADD = 1013904223
HASH_MIX = 1103515245


def plan():
    tasks = []
    for mz in range(H):
        for my in range(H):
            along_y = mz + my > 1 or my > mz
            along_z = mz + my > 1 or mz > my
            for fz in (mz,) if along_z else (mz, -1 - mz):
                for fy in (my,) if along_y else (my, -1 - my):
                    tasks.append((fz, fy, along_y, along_z))

    def hops(task):
        return sum(f if f >= 0 else -f for f in task[:2])

    return sorted(tasks, key=lambda task: (-hops(task), task))


TASKS = plan()
N = len(TASKS)
OF = [
    list(range(N)),
    [i for i in range(N) if TASKS[i][2]],
    [i for i in range(N) if TASKS[i][3]],
    [i for i in range(N) if TASKS[i][2] and TASKS[i][3]],
]
WAVES = [range(N * w // 4, N * (w + 1) // 4) for w in range(4)]
SIZES = [len(OF[q]) for q in (0, 1, 1, 2, 2, 3, 3, 0)]
BASE = [sum(SIZES[:j]) for j in range(8)]
FIRST = (0.5, 1.0, 0.4, 1.0)
SENDS = [
    [(q, i) for i in range(N) for q in (3, 1, 2, 0) if i in OF[q] and (OF[q].index(i) < FIRST[q] * len(OF[q])) == early]
    for early in (True, False)
]


def kernel(
    g_hbm, off_hbm, rx, rstep,
    gv, rp, offv, roff, toff, codes, noise, pm, mxs, rm1, mxs2, rm2, stp_s, scl, sums, rc,
    ld, lo, so, ro, sraw, rr, sm1, sr1, sm2, sr2, s1, r1, sx, rxs,
):
    z, y, c, x = (lax.axis_index(n) for n in ("dp_0", "dp_1", "dp_2", "expert"))

    def rdma(src, dst, send, recv, dev):
        return pltpu.make_async_remote_copy(
            src_ref=src, dst_ref=dst, send_sem=send, recv_sem=recv, device_id=dev, device_id_type=MESH
        )

    partner = (z, y, 1 - c, x)
    per = A // CHUNKS

    def way(position, core):
        return 2 * ((position + core) & 1) - 1

    def load(q, h):
        rows = pl.ds(q * per, per)
        return pltpu.make_async_copy(g_hbm.at[rows, :, h], gv.at[h, rows], ld.at[q, h])

    load_off = pltpu.make_async_copy(off_hbm, offv, lo.at[0])
    load_off.start()
    for q in range(CHUNKS):
        for h in range(2):
            load(q, h).start()

    barrier = pltpu.get_barrier_semaphore()
    me16 = y * 2 + c
    mz16 = z * 2 + c

    def greet(dev):
        pl.semaphore_signal(barrier, inc=1, device_id=dev, device_id_type=MESH)

    def greet16(k, carry):
        p = (me16 + k) & 15
        greet((z, p >> 1, p & 1, x))
        return carry

    def greet14(k, carry):
        p = (mz16 + k) & 15

        @pl.when((p >> 1) != z)
        def _():
            greet((p >> 1, y, p & 1, x))

        return carry

    def greet4(k, carry):
        greet((z, y, c, (x + k) & 3))
        return carry

    def near(position, core):
        return (position - way(position, core)) & 7

    far = sorted(range(1, 2 * A), key=lambda k: -min(k, 2 * A - k))
    for k in far:
        greet14(k, 0)
        greet16(k, 0)
    lax.fori_loop(1, X, greet4, 0)
    greet((near(z, c), near(y, c), c, x))
    greet((near(z, c), near(y, c), 1 - c, x))
    greet((near(z, 1 - c), near(y, 1 - c), 1 - c, x))

    for q in range(CHUNKS):
        for h in range(2):
            load(q, h).wait()

            def block_max(i, carry):
                v = jnp.abs(gv[h, i >> 3, i & 7].astype(jnp.float32))
                m = v[:, :128]
                for t in range(1, TILES):
                    m = jnp.maximum(m, v[:, t * 128 : (t + 1) * 128])
                pm[pl.ds((h * A * A + i) * ROWS, ROWS), :] = m
                return carry

            lax.fori_loop(q * per * A, (q + 1) * per * A, block_max, 0, unroll=4)
    top = pm[pl.ds(0, 128, stride=ROWS), :]
    for r in range(1, ROWS):
        top = jnp.maximum(top, pm[pl.ds(r, 128, stride=ROWS), :])
    mine = jnp.max(top.T, axis=0, keepdims=True)
    mxs[...] = mine
    rm1[me16] = mine
    load_off.wait()

    pl.semaphore_wait(barrier, (2 * A - 1) + (2 * A - 2) + (X - 1) + 3)

    def send_max(k, carry):
        p = (y + k) & 7

        @pl.when(k + 1 - c != 0)
        def _():
            rdma(mxs, rm1.at[me16], sm1.at[0], sr1.at[0], (z, p, 1, x)).start()

        return carry

    lax.fori_loop(0, A, send_max, 0)

    def to_near(core, q):
        return (near(z, core) if q > 1 else z, y if q == 2 else near(y, core), core, x)

    def dest(position, core, f):
        return (position + way(position, core) * f) & 7

    def spot(i, core=c, q=0):
        fz, fy = TASKS[i][:2]
        return dest(z, core, -1 - fz if q > 1 else fz), dest(y, core, -1 - fy if q in (1, 3) else fy)

    sources = [(0, 0)] + [(q, k) for q in (1, 2, 3) for k in range(2)]

    rdma(offv, roff.at[0], so.at[0], ro.at[0], partner).start()
    for core in range(2):
        for q in (1, 2, 3):
            slot = 2 * q - 1 + c
            rdma(offv, roff.at[slot], so.at[3 * core + q], ro.at[slot], to_near(core, q)).start()

    def raw_send(q, i):
        wave = [w for w in range(len(WAVES)) if i in WAVES[w]][0]
        if q == 0:
            zp, yp = spot(i, 1 - c)
            rdma(gv.at[1 - c, zp, yp], rp.at[i], sraw.at[0], rr.at[wave], partner).start()
            return
        n = OF[q].index(i)
        for core in range(2):
            zp, yp = spot(i, core, q)
            rdma(
                gv.at[core, zp, yp], rp.at[BASE[2 * q - 1] + c * len(OF[q]) + n], sraw.at[0], rr.at[wave], to_near(core, q)
            ).start()

    for q, i in SENDS[0]:
        raw_send(q, i)

    lane = lax.broadcasted_iota(jnp.int32, (ROWS, 128), 1)
    column = [(lane + t * 128) * HASH_MUL for t in range(TILES)]

    def dither(j, value):
        start = value * HASH_MUL + HASH_ADD
        toff[...] = jnp.concatenate([start] * 16, axis=0).T
        q = 0 if j == 7 else sources[j][0]
        for n, i in enumerate(OF[q]):
            zp, yp = spot(i)
            tile = toff[pl.ds((yp * 2 + c) * ROWS, ROWS), :]
            index = jnp.full((ROWS, 128), zp, jnp.int32)
            codes[n] = jnp.take_along_axis(tile, index, axis=1, mode="promise_in_bounds")

        def one(n, carry):
            code = codes[n]
            for t in range(TILES):
                v = code + column[t]
                v = v ^ (v >> 13)
                v = v * HASH_MIX
                v = v ^ (v >> 16)
                noise[BASE[j] + n, :, pl.ds(t * 128, 128)] = v & 0xFF000
            return carry

        lax.fori_loop(0, len(OF[q]), one, 0)

    dither(7, offv[...])

    @pl.when(c == 1)
    def _():
        others = rm1.at[pl.ds(0, 2 * A - 1)]
        rdma(others, others, sm1.at[0], sr1.at[0], partner).wait_recv()
        ring = jnp.max(rm1[...], axis=0)
        mxs2[...] = ring
        rm2[z] = ring

        def send_max2(k, carry):
            p = (mz16 + k) & 15
            rdma(mxs2, rm2.at[z], sm2.at[0], sr2.at[0], (p >> 1, y, p & 1, x)).start()
            return carry

        lax.fori_loop(1, 2 * A, send_max2, 0)

    for q, i in SENDS[1]:
        raw_send(q, i)
    for j in range(7):
        rdma(offv, roff.at[j], so.at[0], ro.at[j], partner).wait_recv()
        dither(j, roff[j])

    for core in range(2):

        @pl.when(c == core)
        def _():
            others = rm2.at[pl.ds(0, A - core)]
            rdma(others, others, sm2.at[0], sr2.at[0], partner).wait_recv()

    best = jnp.broadcast_to(jnp.max(rm2[...], axis=0), (ROWS, 128))
    step = jnp.full((ROWS, 128), 2.0 ** (low_power - 6), jnp.float32)
    inverse = jnp.full((ROWS, 128), 2.0 ** (6 - low_power + 20), jnp.float32)
    for e in range(low_power, high_power):
        over = best >= 2.0**e
        step = jnp.where(over, jnp.float32(2.0 ** (e - 5)), step)
        inverse = jnp.where(over, jnp.float32(2.0 ** (25 - e)), inverse)

    def pick(value, block):
        index = jnp.full((ROWS, 128), block, jnp.int32)
        return jnp.take_along_axis(value, index, axis=1, mode="promise_in_bounds")

    for i in range(N):
        zp, yp = spot(i)
        scl[i] = pick(inverse, c * A * A + zp * A + yp)
    stp_s[...] = pick(step, c * A * A + z * A + y)

    def sum_send(i):
        zp, yp = spot(i)
        return rdma(sums.at[i], rc.at[i], s1.at[0], r1.at[0 if i < N // 2 else 1], (zp, yp, c, x))

    for wave in range(len(WAVES)):
        arrived = rp.at[pl.ds(0, sum(i in WAVES[wave] for q, _ in sources for i in OF[q]))]
        rdma(arrived, arrived, sraw.at[0], rr.at[wave], partner).wait_recv()
        for i in WAVES[wave]:
            zp, yp = spot(i)
            scale = scl[i]
            parts = [(gv.at[c, zp, yp], BASE[7] + i)]
            for j in range(7):
                q = sources[j][0]
                if i in OF[q]:
                    n = OF[q].index(i)
                    parts.append((rp.at[BASE[j] + n], BASE[j] + n))

            def tile(t, carry):
                cols = pl.ds(pl.multiple_of(t * 128, 128), 128)
                both = None
                for rows, n in parts:
                    whole = jnp.floor(rows[:, cols].astype(jnp.float32) * scale).astype(jnp.int32)
                    part = (whole + noise[n, :, cols]) >> 20
                    both = part if both is None else both + part
                sums[i, :, cols] = both.astype(jnp.int16)
                return carry

            lax.fori_loop(0, TILES, tile, 0, unroll=True)
            if i < N - 1:
                sum_send(i).start()

    total = sums[N - 1].astype(jnp.int32)
    for part, rows in enumerate((range(N // 2), range(N // 2, N - 1))):
        half = rc.at[pl.ds(rows[0], len(rows))]
        rdma(half, half, s1.at[0], r1.at[part], partner).wait_recv()
        for i in rows:
            total += rc[i].astype(jnp.int32)
    rx[x] = total.astype(jnp.int16)
    rstep[x] = stp_s[...]

    def send_x(k, carry):
        xp = (x + k) & 3
        rdma(rx.at[x], rx.at[x], sx.at[0], rxs.at[0], (z, y, c, xp)).start()
        rdma(rstep.at[x], rstep.at[x], sx.at[1], rxs.at[1], (z, y, c, xp)).start()
        return carry

    for k in (2, 1, 3):
        send_x(k, 0)

    for i in range(7):
        rdma(offv, roff.at[i], so.at[i], ro.at[i], partner).wait_send()
    rdma(rp, rp, sraw.at[0], rr.at[0], partner).wait_send()
    rdma(rc.at[pl.ds(0, N - 1)], rc.at[pl.ds(0, N - 1)], s1.at[0], r1.at[0], partner).wait_send()

    for core in range(2):

        @pl.when(c == core)
        def _():
            others = rm2.at[pl.ds(0, A - core)]
            rdma(others, others, sm1.at[0], sr2.at[0], partner).wait_send()
            if core:
                others = rm1.at[pl.ds(0, 2 * A - 1)]
                rdma(others, others, sm2.at[0], sr1.at[0], partner).wait_send()

    for n, ref in enumerate((rx, rstep)):
        others = ref.at[pl.ds(0, X - 1)]
        rdma(others, others, sx.at[n], rxs.at[n], partner).wait_recv()
        rdma(others, others, sx.at[n], rxs.at[n], partner).wait_send()


def finish(rx, rstep, se_ref, mw_ref, mean_o, new_o, step_o):
    x = lax.axis_index("expert")
    total = rx[X - 1].astype(jnp.int32)
    step = rstep[X - 1]
    for s in range(X - 1):
        here = se_ref[:, s : s + 1] == x
        total = jnp.where(here, rx[s].astype(jnp.int32), total)
        step = jnp.where(here, rstep[s], step)
    share = step * (1.0 / (2 * A * A))
    total = total.astype(jnp.float32)
    for t in range(TILES):
        cols = slice(t * 128, (t + 1) * 128)
        mean = total[:, cols] * share
        mean_o[:, cols] = mean
        new_o[:, cols] = mw_ref[:, cols] - learn_rate * mean
    step_o[...] = step[0:1, 0:1]


def body(expert_grads, round_offsets, slot_expert, master_weight):
    f32, bf16, i32 = jnp.float32, jnp.bfloat16, jnp.int32
    dma = pltpu.SemaphoreType.DMA
    vmem = pl.BlockSpec(memory_space=pltpu.VMEM)
    hbm = pl.BlockSpec(memory_space=pl.ANY)
    gathered, steps = pl.pallas_call(
        kernel,
        name="average",
        out_shape=(pltpu.VMEM((X, ROWS, COLS), jnp.int16), pltpu.VMEM((X, ROWS, 128), f32)),
        in_specs=[hbm, hbm],
        out_specs=(vmem, vmem),
        scratch_shapes=[
            pltpu.VMEM((2, A, A, ROWS, COLS), bf16),
            pltpu.VMEM((BASE[7], ROWS, COLS), bf16),
            pltpu.VMEM((A, 128), i32),
            pltpu.VMEM((7, A, 128), i32),
            pltpu.VMEM((128, 128), i32),
            pltpu.VMEM((N, ROWS, 128), i32),
            pltpu.VMEM((sum(SIZES), ROWS, COLS), i32),
            pltpu.VMEM((2 * A * A * ROWS, 128), f32),
            pltpu.VMEM((1, 128), f32),
            pltpu.VMEM((2 * A, 1, 128), f32),
            pltpu.VMEM((1, 128), f32),
            pltpu.VMEM((A, 1, 128), f32),
            pltpu.VMEM((ROWS, 128), f32),
            pltpu.VMEM((N, ROWS, 128), f32),
            pltpu.VMEM((N, ROWS, COLS), jnp.int16),
            pltpu.VMEM((N, ROWS, COLS), jnp.int16),
            dma((CHUNKS, 2)),
            dma((1,)),
            dma((7,)),
            dma((7,)),
            dma((1,)),
            dma((len(WAVES),)),
            dma((1,)),
            dma((1,)),
            dma((1,)),
            dma((1,)),
            dma((1,)),
            dma((2,)),
            dma((2,)),
            dma((2,)),
        ],
        compiler_params=pltpu.CompilerParams(collective_id=0, has_side_effects=True),
    )(expert_grads.reshape(A, A, 2, ROWS, COLS), round_offsets.reshape(A, 128))
    mean, new, step = pl.pallas_call(
        finish,
        name="finish",
        out_shape=(
            jax.ShapeDtypeStruct((ROWS, COLS), f32),
            jax.ShapeDtypeStruct((ROWS, COLS), f32),
            jax.ShapeDtypeStruct((1, 1), f32),
        ),
        in_specs=[vmem, vmem, vmem, vmem],
        out_specs=(vmem, vmem, vmem),
        compiler_params=pltpu.CompilerParams(vmem_limit_bytes=1024 * 1024),
    )(gathered, steps, slot_expert.reshape(1, X), master_weight.reshape(ROWS, COLS))
    return mean[None], new[None], step


def solution(mesh):
    finer = Mesh(
        mesh.devices.reshape(A, A, 2, mesh.shape["expert"]), ("dp_0", "dp_1", "dp_2", "expert")
    )
    return jax.shard_map(
        body,
        mesh=finer,
        in_specs=(P(DP, "expert", None, None), P(DP, "expert", None), P(), P("expert", DP, None)),
        out_specs=(P("expert", DP, None), P("expert", DP, None), P("expert", DP)),
        check_vma=False,
    )
```
